32 devices in a mesh: parts: 2 (over y), pix: 4 (over z), par: 4 (over x, core).
Axes of the slice: x: 2, y: 2, z: 4, core: 2. Of those that a mesh axis runs over, the one named last changes fastest.
Arguments:
- green_matrix: bfloat16 [4608, 16384], P('pix', 'par'), may hold values from -0.046875 to 0.046875
- observed: bfloat16 [64, 4608], P('parts', 'pix'), parts along dimension 0, may hold values from -1000 to 1000
Outputs:
- solution: float32 [64, 16384], P('parts', 'par'), parts along dimension 0
- residual: float32 [64, 4608], P('parts', 'pix'), parts along dimension 0
The draws below stay inside these ranges and needn't reach their ends.
There are 2 independent parts, one for each index of `parts`. The reference program is written for one: setup_inputs(seed, part) draws one part's arguments, and reference() takes and returns one part's arrays. A program takes and returns all parts, laid end to end along the dimension named above; an argument that names none is the same for every part. Nothing has to cross between parts.
All inputs are finite; a program needn't handle non-finite values.
Results may differ from the reference program's by a relative error of at most 0.0038.
Values may be sent and summed in bfloat16 or wider, within the bound.
No kernel may reach another device: no remote copies, remote signals or barrier semaphores. Data moves between devices by JAX's collectives and lax.ppermute only.
A program may use at most 64 MiB of HBM per device.

```python
import math
import jax
import jax.numpy as jnp
from jax import lax

GRID = 128
PARAMS = 16384
SETS = 32
PIXELS = 4608
ITERS = 5


def draw_green_matrix(key, part):
    keys = jax.random.split(jax.random.fold_in(key, 29), 4)
    base = jnp.clip(jax.random.normal(keys[0], (PIXELS, PARAMS), jnp.float32), -6.0, 6.0)
    column_scale = jnp.exp(jax.random.uniform(keys[1], (1, PARAMS), jnp.float32, -2.5, 0.0))
    left = jax.random.normal(keys[2], (PIXELS, 3), jnp.float32)
    right = jax.random.normal(keys[3], (3, PARAMS), jnp.float32)
    common = left[:, 0:1] * right[0:1, :] + left[:, 1:2] * right[1:2, :] + left[:, 2:3] * right[2:3, :]
    common = common / math.sqrt(3.0)
    place = jnp.arange(PARAMS, dtype=jnp.float32)[None, :] / PARAMS - 1.0
    rising = jnp.exp(math.log(3.0) * place)
    value = (base + 0.06 * common) * column_scale * rising * (2.2 / GRID)
    bound = 6.0 / GRID
    return jnp.clip(value, -bound, bound).astype(jnp.bfloat16)


def draw_observed(key, part):
    keys = jax.random.split(jax.random.fold_in(key, 71), 3)
    position = jnp.arange(PIXELS, dtype=jnp.float32) / PIXELS
    base = jnp.clip(jax.random.normal(keys[0], (SETS, PIXELS), jnp.float32), -6.0, 6.0)
    rising = jnp.exp(math.log(3.0) * position)[None, :]
    row_scale = jnp.exp(jax.random.uniform(keys[1], (1, PIXELS), jnp.float32, math.log(0.5), math.log(5.0)))
    set_scale = jnp.exp(jax.random.uniform(keys[2], (SETS, 1), jnp.float32, math.log(0.3), math.log(3.0)))
    return (base * rising * row_scale * set_scale).astype(jnp.bfloat16)


def setup_inputs(seed: int = 0, part: int = 0) -> dict:
    seeds = jax.random.split(jax.random.key(seed), 3)
    own_keys = jax.random.split(jax.random.fold_in(seeds[2], part), 3)
    green_matrix = draw_green_matrix(jax.random.fold_in(seeds[2], 71), part)
    observed = draw_observed(jax.random.fold_in(jax.random.fold_in(seeds[2], part), 71), part)
    return {"green_matrix": green_matrix, "observed": observed}


def smooth(values):
    set_count = values.shape[0]
    tiles = values.reshape(set_count, GRID, GRID)
    padded = jnp.pad(tiles, ((0, 0), (1, 1), (1, 1)))
    beside_all = padded[:, 2:, 1:-1] + padded[:, :-2, 1:-1] + padded[:, 1:-1, 2:] + padded[:, 1:-1, :-2]
    return (0.25 * (4.0 * tiles - beside_all)).reshape(set_count, GRID * GRID)


def reference(green_matrix, observed):
    residual = observed.astype(jnp.float32)
    gradient = jnp.dot(observed, green_matrix, preferred_element_type=jnp.float32)
    grad_sq = jnp.sum(gradient * gradient, axis=1)
    direction = gradient
    solution = jnp.zeros((SETS, GRID * GRID), jnp.float32)
    smooth_res = jnp.zeros((SETS, GRID * GRID), jnp.float32)
    for sweep in range(ITERS):
        rounded = direction.astype(jnp.bfloat16)
        image = lax.dot_general(rounded, green_matrix, (((1,), (1,)), ((), ())), preferred_element_type=jnp.float32)
        smoothed = smooth(lax.optimization_barrier(rounded).astype(jnp.float32))
        curvature = jnp.sum(image * image, axis=1) + jnp.sum(smoothed * smoothed, axis=1)
        step_len = (grad_sq / curvature)[:, None]
        solution = solution + step_len * direction
        residual = residual - step_len * image
        smooth_res = smooth_res - step_len * smoothed
        if sweep + 1 < ITERS:
            gradient = jnp.dot(residual.astype(jnp.bfloat16), green_matrix, preferred_element_type=jnp.float32) + smooth(smooth_res)
            fresh_sq = jnp.sum(gradient * gradient, axis=1)
            direction = gradient + (fresh_sq / grad_sq)[:, None] * direction
            grad_sq = fresh_sq
    return solution, residual
```

```python
import jax
import jax.numpy as jnp
from jax import lax
from jax.sharding import PartitionSpec as P

GRID = 128
ITERS = 5
LANES = 128
BF16 = jnp.bfloat16
F32 = jnp.float32


def xor_pairs(count, offset):
    return [(i, i ^ offset) for i in range(count)]


def split3(values):
    high = lax.reduce_precision(values, 8, 7)
    rest = values - high
    mid = lax.reduce_precision(rest, 8, 7)
    low = lax.reduce_precision(rest - mid, 8, 7)
    return high.astype(BF16), mid.astype(BF16), low.astype(BF16)


def join3(terms):
    high, mid, low = (term.astype(F32) for term in terms)
    return (high + mid) + low


def pack_scalars(columns):
    terms = [term[:, None] for column in columns for term in split3(column)]
    block = jnp.concatenate(terms, axis=1)
    return jnp.pad(block, ((0, 0), (0, LANES - block.shape[1])))


def unpack_scalars(block, count):
    return [join3([block[:, 3 * i + t] for t in range(3)]) for i in range(count)]


def tree_sum(parts):
    while len(parts) > 1:
        parts = [parts[i] + parts[i + 1] for i in range(0, len(parts), 2)]
    return parts[0]


def beside(row):
    padded = jnp.pad(row, ((0, 0), (0, 0), (1, 1)))
    return padded[:, :, 2:] + padded[:, :, :-2]


def inner_smooth(tiles):
    mid = tiles[:, 1:-1]
    return mid - 0.25 * ((tiles[:, 2:] + tiles[:, :-2]) + beside(mid))


def seam(lower, upper):
    low0, low1 = lower[:, :1], lower[:, 1:]
    up0, up1 = upper[:, :1], upper[:, 1:]
    low_s = low1 - 0.25 * (low0 + beside(low1))
    up_s = up0 - 0.25 * (up1 + beside(up0))
    cross = -0.5 * (low_s * up0 + up_s * low1)
    return jnp.sum(cross + 0.0625 * (up0 * up0 + low1 * low1), axis=(1, 2))


def gather_pix(shard, count):
    index = lax.axis_index("pix")
    parts = [shard]
    for offset in range(1, count):
        parts.append(lax.ppermute(shard, "pix", xor_pairs(count, offset)))
    step = 1
    while step < count:
        swap = (index // step) % 2 == 1
        parts = [jnp.where(swap, parts[i ^ step], parts[i]) for i in range(count)]
        step *= 2
    return jnp.concatenate(parts, axis=1)


def par_sum(value, scalars, first, last, count):
    sets, width = value.shape
    index = lax.axis_index("par")
    rows = first.shape
    above = jnp.zeros(rows, F32)
    below = jnp.zeros(rows, F32)
    step = 1
    while step < count:
        upper_side = (index // step) % 2 == 1
        inside = index % step
        flat = [first.reshape(sets, -1), last.reshape(sets, -1)]
        if step == 1:
            packed = jnp.stack(scalars, axis=1)
            packed = jnp.pad(packed, ((0, 0), (0, LANES - packed.shape[1])))
            message = jnp.concatenate([value, packed] + flat, axis=1)
        else:
            message = jnp.concatenate(
                [value.astype(BF16), pack_scalars(scalars)] + [rows_.astype(BF16) for rows_ in flat], axis=1
            )
        got = lax.ppermute(message, "par", xor_pairs(count, step))
        if step == 1:
            value = value + got[:, :width]
            others = [got[:, width + i] for i in range(len(scalars))]
        else:
            value = message[:, :width].astype(F32) + got[:, :width].astype(F32)
            others = unpack_scalars(got[:, width : width + LANES], len(scalars))
        got_rows = got[:, width + LANES :].astype(F32)
        half = got_rows.shape[1] // 2
        got_first = got_rows[:, :half].reshape(rows)
        got_last = got_rows[:, half:].reshape(rows)
        lower_last = jnp.where(upper_side, got_last, last)
        upper_first = jnp.where(upper_side, first, got_first)
        scalars = [mine + other for mine, other in zip(scalars, others)]
        scalars[1] = scalars[1] + seam(lower_last, upper_first)
        above = jnp.where(upper_side & (inside == 0), lower_last, above)
        below = jnp.where(jnp.logical_not(upper_side) & (inside == step - 1), upper_first, below)
        first = jnp.where(upper_side, got_first, first)
        last = jnp.where(upper_side, last, got_last)
        step *= 2
    return value, scalars, above, below


def on_device(green_matrix, observed):
    sets = observed.shape[0]
    pixels, cells = green_matrix.shape
    n_pix, n_par = lax.axis_size("pix"), lax.axis_size("par")
    here, tile = lax.axis_index("pix"), lax.axis_index("par")
    width = cells // n_pix
    rows = cells // GRID
    direct = n_pix <= 8

    def block_of(whole, offset):
        return lax.dynamic_slice_in_dim(whole, (here ^ offset) * width, width, axis=1)

    own_mask = (jnp.arange(cells) // width == here)[None, :]

    def scatter_pix(partial, scalar):
        if not direct:
            shard = lax.psum_scatter(partial, "pix", scatter_dimension=1, tiled=True)
            return shard, lax.psum(scalar, "pix"), jnp.zeros_like(partial)
        rounded = lax.reduce_precision(partial, 8, 7)
        lost = jnp.where(own_mask, 0.0, partial - rounded)
        sent = rounded.astype(BF16)
        tail = pack_scalars([scalar])
        shards, totals = [block_of(partial, 0)], [scalar]
        for offset in range(1, n_pix):
            message = jnp.concatenate([block_of(sent, offset), tail], axis=1)
            got = lax.ppermute(message, "pix", xor_pairs(n_pix, offset))
            shards.append(got[:, :width].astype(F32))
            totals.append(unpack_scalars(got[:, width:], 1)[0])
        return tree_sum(shards), tree_sum(totals), lost

    def gather(shard):
        if direct:
            return gather_pix(shard, n_pix)
        return lax.all_gather(shard, "pix", axis=1, tiled=True)

    residual = observed.astype(F32)
    partial = jnp.dot(observed, green_matrix, preferred_element_type=F32)
    zero_set = jnp.zeros((sets,), F32)
    grad, _, lost = scatter_pix(partial, zero_set)
    solution = jnp.zeros((sets, cells), F32)
    for sweep in range(ITERS):
        whole = gather(grad.astype(BF16))
        fresh = whole.astype(F32)
        tiles = fresh.reshape(sets, rows, GRID)
        image = lax.dot_general(whole, green_matrix, (((1,), (1,)), ((), ())), preferred_element_type=F32)
        alone = inner_smooth(jnp.pad(tiles, ((0, 0), (1, 1), (0, 0))))
        scalars = [jnp.sum(fresh * fresh, axis=1), jnp.sum(alone * alone, axis=(1, 2))]
        if sweep:
            scalars.append(jnp.sum(tiles * twice, axis=(1, 2)))
        image, scalars, above, below = par_sum(image, scalars, tiles[:, :2], tiles[:, -2:], n_par)
        padded = jnp.concatenate([above, tiles, below], axis=1)
        if sweep:
            beta = scalars[0] / grad_sq
            forward = image + beta[:, None] * forward
            direction = padded + beta[:, None, None] * direction
            smooth_sq = scalars[1] + 2.0 * beta * scalars[2] + beta * beta * smooth_sq
        else:
            forward, direction, smooth_sq = image, padded, scalars[1]
        grad_sq = scalars[0]
        image_sq = jnp.sum(forward * forward, axis=1)
        if sweep + 1 < ITERS:
            once = inner_smooth(direction)
            row_id = jnp.arange(rows + 2)[None, :, None]
            outside = ((row_id == 0) & (tile == 0)) | ((row_id == rows + 1) & (tile == n_par - 1))
            twice = inner_smooth(jnp.where(outside, 0.0, once))
            partial = jnp.dot(forward.astype(BF16), green_matrix, preferred_element_type=F32)
            guess = (n_pix * image_sq + smooth_sq) / grad_sq
            aimed = partial - guess[:, None] * lost
            change, image_sq, dropped = scatter_pix(aimed, image_sq)
            change = change + block_of(twice.reshape(sets, cells), 0)
        elif direct:
            tail = pack_scalars([image_sq])
            totals = [image_sq]
            for offset in range(1, n_pix):
                got = lax.ppermute(tail, "pix", xor_pairs(n_pix, offset))
                totals.append(unpack_scalars(got, 1)[0])
            image_sq = tree_sum(totals)
        else:
            image_sq = lax.psum(image_sq, "pix")
        step_len = (grad_sq / (image_sq + smooth_sq))[:, None]
        solution = solution + step_len * direction[:, 2:-2].reshape(sets, cells)
        residual = residual - step_len * forward
        if sweep + 1 < ITERS:
            lost = lost - step_len * (partial - aimed + dropped)
            grad = grad - step_len * change
    return (solution, residual)


def solution(mesh):
    return jax.shard_map(
        on_device,
        mesh=mesh,
        in_specs=(P("pix", "par"), P("parts", "pix")),
        out_specs=(P("parts", "par"), P("parts", "pix")),
        check_vma=False,
    )
```

```python
import functools

import jax
import jax.numpy as jnp
from jax import lax
from jax.experimental import pallas as pl
from jax.experimental.pallas import tpu as pltpu
from jax.sharding import PartitionSpec as P

GRID = 128
ITERS = 5
LANES = 128
EDGE = 2 * GRID
SLOTS = 8
BF16 = jnp.bfloat16
F32 = jnp.float32

GRAD_SQ, SMOOTH_SQ, CROSS = 0, 1, 2
IMAGE_SQ = 2
STEP = 3


def xor_pairs(count, offset):
    return [(i, i ^ offset) for i in range(count)]


def tree_sum(parts):
    while len(parts) > 1:
        parts = [parts[i] + parts[i + 1] for i in range(0, len(parts), 2)]
    return parts[0]


def lane_ids(sets):
    return lax.broadcasted_iota(jnp.int32, (sets, LANES), 1)


def beside(row):
    lane = lane_ids(row.shape[0])
    left = jnp.where(lane == 0, 0.0, pltpu.roll(row, 1, 1))
    right = jnp.where(lane == LANES - 1, 0.0, pltpu.roll(row, LANES - 1, 1))
    return left + right


def smooth_row(above, row, below):
    near = beside(row)
    if above is not None:
        near = near + above
    if below is not None:
        near = near + below
    return row - 0.25 * near


def lanes_of(columns, sets):
    lane = lane_ids(sets)
    block = jnp.zeros((sets, LANES), F32)
    for slot, column in columns.items():
        block = jnp.where(lane == slot, column, block)
    return block


def pack(block):
    block = jnp.where(lane_ids(block.shape[0]) < SLOTS, block, 0.0)
    high = block.astype(BF16).astype(F32)
    rest = block - high
    mid = rest.astype(BF16).astype(F32)
    low = (rest - mid).astype(BF16).astype(F32)
    return (high + pltpu.roll(mid, SLOTS, 1) + pltpu.roll(low, 2 * SLOTS, 1)).astype(BF16)


def unpack(packed):
    block = packed.astype(F32)
    mid = pltpu.roll(block, LANES - SLOTS, 1)
    low = pltpu.roll(block, LANES - 2 * SLOTS, 1)
    return jnp.where(lane_ids(block.shape[0]) < SLOTS, (block + mid) + low, 0.0)


def row_of(values, index):
    return values[:, index * GRID : (index + 1) * GRID]


def seam(lower, upper):
    low0, low1, up0, up1 = row_of(lower, 0), row_of(lower, 1), row_of(upper, 0), row_of(upper, 1)
    cross = smooth_row(low0, low1, None) * up0 + smooth_row(None, up0, up1) * low1
    return jnp.sum(0.0625 * (up0 * up0 + low1 * low1) - 0.5 * cross, axis=1, keepdims=True)


def merge(mine_ref, got_ref, above, below, pixels, step, tile):
    upper_side = (tile // step) % 2 == 1
    inside = tile % step
    scalar_at, row_at = pl.ds(pixels, LANES), pl.ds(pixels + LANES, 2 * EDGE)
    if mine_ref.dtype == F32:
        mine, got = mine_ref[:, scalar_at], got_ref[:, scalar_at]
    else:
        mine, got = unpack(mine_ref[:, scalar_at]), unpack(got_ref[:, scalar_at])
    edges, got_edges = mine_ref[:, row_at].astype(F32), got_ref[:, row_at].astype(F32)
    first = jnp.where(upper_side, got_edges[:, :EDGE], edges[:, :EDGE])
    last = jnp.where(upper_side, edges[:, EDGE:], got_edges[:, EDGE:])
    lower_last = jnp.where(upper_side, got_edges[:, EDGE:], edges[:, EDGE:])
    upper_first = jnp.where(upper_side, edges[:, :EDGE], got_edges[:, :EDGE])
    sets = mine.shape[0]
    scalars = mine + got + lanes_of({SMOOTH_SQ: seam(lower_last, upper_first)}, sets)
    above = jnp.where(upper_side & (inside == 0), lower_last, above)
    below = jnp.where(jnp.logical_not(upper_side) & (inside == step - 1), upper_first, below)
    value = mine_ref[:, :pixels].astype(F32) + got_ref[:, :pixels].astype(F32)
    return value, scalars, first, last, above, below


def forward_kernel(n_shards, first_sweep, *refs):
    shards, refs = refs[:n_shards], refs[n_shards:]
    if first_sweep:
        green, whole, message = refs
    else:
        twice, green, whole, message = refs
    sets, cells = whole.shape
    width = cells // n_shards
    pixels = green.shape[0]
    here = lax.axis_index("pix")
    image = jnp.zeros((sets, pixels), F32)
    for offset, shard in enumerate(shards):
        at = pl.ds(pl.multiple_of((here ^ offset if n_shards > 1 else 0) * width, LANES), width)
        value = shard[...]
        whole[:, at] = value
        image += lax.dot_general(value, green[:, at], (((1,), (1,)), ((), ())), preferred_element_type=F32)
    message[:, :pixels] = image
    rows = cells // GRID
    grad_sq = jnp.zeros((sets, LANES), F32)
    smooth_sq = jnp.zeros((sets, LANES), F32)
    cross = jnp.zeros((sets, LANES), F32)
    above, row = None, whole[:, :GRID].astype(F32)
    for r in range(rows):
        below = whole[:, (r + 1) * GRID : (r + 2) * GRID].astype(F32) if r + 1 < rows else None
        alone = smooth_row(above, row, below)
        grad_sq += row * row
        smooth_sq += alone * alone
        if not first_sweep:
            cross += row * twice[:, r * GRID : (r + 1) * GRID]
        above, row = row, below
    columns = {GRAD_SQ: jnp.sum(grad_sq, axis=1, keepdims=True), SMOOTH_SQ: jnp.sum(smooth_sq, axis=1, keepdims=True)}
    if not first_sweep:
        columns[CROSS] = jnp.sum(cross, axis=1, keepdims=True)
    message[:, pixels : pixels + LANES] = lanes_of(columns, sets)
    message[:, pixels + LANES : pixels + LANES + EDGE] = whole[:, :EDGE].astype(F32)
    message[:, pixels + LANES + EDGE :] = whole[:, cells - EDGE :].astype(F32)


def middle_kernel(step, *refs):
    if step == 1:
        mine, got, message, above, below = refs
        old_above = old_below = jnp.zeros(above.shape, F32)
    else:
        mine, got, above_in, below_in, message, above, below = refs
        old_above, old_below = above_in[...], below_in[...]
    pixels = mine.shape[1] - LANES - 2 * EDGE
    value, scalars, first, last, up, down = merge(mine, got, old_above, old_below, pixels, step, lax.axis_index("par"))
    message[:, :pixels] = value.astype(BF16)
    message[:, pixels : pixels + LANES] = pack(scalars)
    message[:, pixels + LANES : pixels + LANES + EDGE] = first.astype(BF16)
    message[:, pixels + LANES + EDGE :] = last.astype(BF16)
    above[...] = up
    below[...] = down


def advance(step, n_par, first_sweep, need_twice, refs):
    mine, got, above_in, below_in, whole, old_scalars, old_image, old_direction, scalars, image, direction, once, twice = refs
    tile = lax.axis_index("par")
    sets, pixels = image.shape
    cells = whole.shape[1]
    rows = cells // GRID
    value, sums, _, _, above, below = merge(mine, got, above_in[...], below_in[...], pixels, step, tile)
    grad_sq = sums[:, GRAD_SQ : GRAD_SQ + 1]
    smooth_sq = sums[:, SMOOTH_SQ : SMOOTH_SQ + 1]
    if first_sweep:
        image[...] = value
        direction[:, :EDGE] = above
        direction[:, EDGE : EDGE + cells] = whole[...].astype(F32)
        direction[:, EDGE + cells :] = below
    else:
        beta = grad_sq / old_scalars[:, GRAD_SQ : GRAD_SQ + 1]
        old_smooth = old_scalars[:, SMOOTH_SQ : SMOOTH_SQ + 1]
        smooth_sq = smooth_sq + beta * (2.0 * sums[:, CROSS : CROSS + 1] + beta * old_smooth)
        image[...] = value + beta * old_image[...]
        direction[:, :EDGE] = above + beta * old_direction[:, :EDGE]
        direction[:, EDGE : EDGE + cells] = whole[...].astype(F32) + beta * old_direction[:, EDGE : EDGE + cells]
        direction[:, EDGE + cells :] = below + beta * old_direction[:, EDGE + cells :]
    image_sq = jnp.zeros((sets, LANES), F32)
    for at in range(0, pixels, LANES):
        part = image[:, at : at + LANES]
        image_sq += part * part
    image_sq = jnp.sum(image_sq, axis=1, keepdims=True)
    scalars[...] = lanes_of({GRAD_SQ: grad_sq, SMOOTH_SQ: smooth_sq, IMAGE_SQ: image_sq}, sets)
    if need_twice:
        def direction_row(r):
            return direction[:, r * GRID : (r + 1) * GRID]

        for r in range(rows + 2):
            row = smooth_row(direction_row(r), direction_row(r + 1), direction_row(r + 2))
            if r == 0:
                row = jnp.where(tile == 0, 0.0, row)
            if r == rows + 1:
                row = jnp.where(tile == n_par - 1, 0.0, row)
            once[:, r * GRID : (r + 1) * GRID] = row

        def once_row(r):
            return once[:, r * GRID : (r + 1) * GRID]

        for r in range(rows):
            twice[:, r * GRID : (r + 1) * GRID] = smooth_row(once_row(r), once_row(r + 1), once_row(r + 2))
    return grad_sq, smooth_sq, image_sq


def send_blocks(image, green, blocks, own, missed, lost, guess, tail):
    here = lax.axis_index("pix")
    width = own.shape[1]
    for offset in range(len(blocks), -1, -1):
        at = pl.ds(pl.multiple_of((here ^ offset) * width, LANES), width)
        part = jnp.dot(image, green[:, at], preferred_element_type=F32)
        if offset == 0:
            own[...] = part
            missed[:, at] = jnp.zeros_like(part)
        else:
            aimed = part if lost is None else part - guess * lost[:, at]
            sent = aimed.astype(BF16)
            blocks[offset - 1][:, :width] = sent
            missed[:, at] = part - sent.astype(F32)
            if tail is not None:
                blocks[offset - 1][:, width:] = tail


def backward_kernel(step, n_pix, n_par, first_sweep, direct, *refs):
    refs = list(refs)
    green = refs.pop(0)
    lost = refs.pop(0) if direct else None
    mine, got, above, below, whole = refs[:5]
    refs = refs[5:]
    if first_sweep:
        olds = [None] * 3
    else:
        olds, refs = refs[:3], refs[3:]
    scalars, image, direction, twice = refs[:4]
    once = refs[-1]
    refs = refs[4:-1]
    sums = advance(
        step, n_par, first_sweep, True,
        [mine, got, above, below, whole, *olds, scalars, image, direction, once, twice],
    )
    rounded = image[...].astype(BF16)
    if not direct:
        refs[0][...] = jnp.dot(rounded, green[...], preferred_element_type=F32)
        return
    grad_sq, smooth_sq, image_sq = sums
    guess = (n_pix * image_sq + smooth_sq) / grad_sq
    own, missed, blocks = refs[0], refs[1], refs[2:]
    send_blocks(rounded, green, blocks, own, missed, lost, guess, pack(scalars[...]))
    width = own.shape[1]
    at = pl.ds(pl.multiple_of(lax.axis_index("pix") * width, LANES), width)
    own[...] += twice[:, at]


def last_kernel(step, n_par, *refs):
    ins, (scalars, image, direction) = refs[:8], refs[8:]
    advance(step, n_par, False, False, [*ins, scalars, image, direction, None, None])


def start_kernel(observed, green, own, missed, *blocks):
    send_blocks(observed[...], green, blocks, own, missed, None, None, None)


def receive_start_kernel(n_got, own, *refs):
    got, (grad, rounded) = refs[:n_got], refs[n_got:]
    value = tree_sum([own[...]] + [ref[...].astype(F32) for ref in got])
    grad[...] = value
    rounded[...] = value.astype(BF16)


def step_length(scalars, totals):
    image_sq = tree_sum(totals)[:, IMAGE_SQ : IMAGE_SQ + 1]
    return scalars[:, GRAD_SQ : GRAD_SQ + 1] / (image_sq + scalars[:, SMOOTH_SQ : SMOOTH_SQ + 1])


def receive_kernel(n_got, own, scalars, old_grad, *refs):
    got, (grad, rounded, length) = refs[:n_got], refs[n_got:]
    width = own.shape[1]
    mine = scalars[...]
    step_len = step_length(mine, [mine] + [unpack(ref[:, width:]) for ref in got])
    change = tree_sum([own[...]] + [ref[:, :width].astype(F32) for ref in got])
    value = old_grad[...] - step_len * change
    grad[...] = value
    rounded[...] = value.astype(BF16)
    length[...] = jnp.broadcast_to(step_len, length.shape)


def update_kernel(has_lost, length, direction, image, solution, residual, *refs):
    step_len = length[:, :1]
    if has_lost:
        lost, missed, new_solution, new_residual, new_lost = refs
        new_lost[...] = lost[...] - step_len * missed[...]
    else:
        new_solution, new_residual = refs
    cells = solution.shape[1]
    new_solution[...] = solution[...] + step_len * direction[:, EDGE : EDGE + cells]
    new_residual[...] = residual[...] - step_len * image[...]


def finish_kernel(n_got, *refs):
    scalars, got = refs[0], refs[1 : 1 + n_got]
    direction, image, solution, residual, new_solution, new_residual = refs[1 + n_got :]
    mine = scalars[...]
    step_len = step_length(mine, [mine] + [ref[...] for ref in got])
    cells = solution.shape[1]
    new_solution[...] = solution[...] + step_len * direction[:, EDGE : EDGE + cells]
    new_residual[...] = residual[...] - step_len * image[...]


def call(kernel, operands, outs, scratch=(), flops=0, limit=24 << 20):
    vmem = pl.BlockSpec(memory_space=pltpu.VMEM)
    shapes = [jax.ShapeDtypeStruct(*out) for out in outs]
    moved = sum(x.size * x.dtype.itemsize for x in [*operands, *shapes])
    return pl.pallas_call(
        kernel,
        in_specs=[vmem] * len(operands),
        out_specs=[vmem] * len(outs),
        out_shape=shapes,
        scratch_shapes=list(scratch),
        compiler_params=pltpu.CompilerParams(vmem_limit_bytes=limit),
        cost_estimate=pl.CostEstimate(flops=flops or moved, bytes_accessed=moved, transcendentals=0),
    )(*operands)


def exchange(blocks, axis, count):
    return [lax.ppermute(block, axis, xor_pairs(count, k + 1)) for k, block in enumerate(blocks)]


def on_device(green, observed):
    sets = observed.shape[0]
    pixels, cells = green.shape
    n_pix, n_par = lax.axis_size("pix"), lax.axis_size("par")
    here = lax.axis_index("pix")
    width = cells // n_pix
    direct = n_pix <= 8 and width % LANES == 0
    flops = 2 * sets * pixels * cells
    block, shard = ((sets, width + LANES), BF16), ((sets, width), F32)
    scalar = ((sets, LANES), F32)
    line, wide, edge = ((sets, pixels), F32), ((sets, cells), F32), ((sets, EDGE), F32)
    ring = ((sets, cells + 2 * EDGE), F32)

    def gather(rounded):
        if direct:
            return [rounded] + exchange([rounded] * (n_pix - 1), "pix", n_pix)
        return [lax.all_gather(rounded, "pix", axis=1, tiled=True)]

    lost = None
    if direct:
        own, lost, *blocks = call(
            start_kernel, [observed, green], [shard, wide] + [((sets, width), BF16)] * (n_pix - 1), flops=flops
        )
        got = exchange(blocks, "pix", n_pix)
    else:
        partial = jnp.dot(observed, green, preferred_element_type=F32)
        own, got = lax.psum_scatter(partial, "pix", scatter_dimension=1, tiled=True), []
    grad, rounded = call(
        functools.partial(receive_start_kernel, len(got)), [own, *got], [shard, ((sets, width), BF16)]
    )
    solution = jnp.zeros((sets, cells), F32)
    residual = observed.astype(F32)
    scalars = image = direction = twice = None
    for sweep in range(ITERS):
        shards = gather(rounded)
        first, final = sweep == 0, sweep + 1 == ITERS
        length_of = pixels + LANES + 2 * EDGE
        whole, message = call(
            functools.partial(forward_kernel, len(shards), first),
            [*shards, *([] if first else [twice]), green],
            [((sets, cells), BF16), ((sets, length_of), F32)],
            flops=flops,
        )
        step, above, below = 1, None, None
        while True:
            got = lax.ppermute(message, "par", xor_pairs(n_par, step))
            if 2 * step >= n_par:
                break
            message, above, below = call(
                functools.partial(middle_kernel, step),
                [message, got, *([] if step == 1 else [above, below])],
                [((sets, length_of), BF16), edge, edge],
            )
            step *= 2
        if above is None:
            above = below = jnp.zeros(edge[0], F32)
        ins = [message, got, above, below, whole, *([] if first else [scalars, image, direction])]
        if final:
            scalars, image, direction = call(
                functools.partial(last_kernel, step, n_par), ins, [scalar, line, ring]
            )
            if direct:
                got = exchange([scalars] * (n_pix - 1), "pix", n_pix)
            else:
                got = []
                scalars = scalars.at[:, IMAGE_SQ].set(lax.psum(scalars[:, IMAGE_SQ], "pix"))
            return tuple(
                call(
                    functools.partial(finish_kernel, len(got)),
                    [scalars, *got, direction, image, solution, residual],
                    [wide, line],
                )
            )
        kernel = functools.partial(backward_kernel, step, n_pix, n_par, first, direct)
        scratch = [pltpu.VMEM((sets, cells + EDGE), F32)]
        outs = [scalar, line, ring, wide]
        if direct:
            scalars, image, direction, twice, own, missed, *blocks = call(
                kernel, [green, lost, *ins], outs + [shard, wide] + [block] * (n_pix - 1), scratch, flops
            )
            got = exchange(blocks, "pix", n_pix)
        else:
            scalars, image, direction, twice, partial = call(kernel, [green, *ins], outs + [wide], scratch, flops)
            own = lax.psum_scatter(partial, "pix", scatter_dimension=1, tiled=True)
            own = own + lax.dynamic_slice_in_dim(twice, here * width, width, axis=1)
            image_sq = lax.psum(scalars[:, IMAGE_SQ], "pix")
            scalars = scalars.at[:, IMAGE_SQ].set(image_sq)
            got = []
        grad, rounded, length = call(
            functools.partial(receive_kernel, len(got)),
            [own, scalars, grad, *got],
            [shard, ((sets, width), BF16), scalar],
        )
        tail = call(
            functools.partial(update_kernel, direct),
            [length, direction, image, solution, residual, *([lost, missed] if direct else [])],
            [wide, line] + ([wide] if direct else []),
        )
        solution, residual = tail[:2]
        lost = tail[2] if direct else None


def solution(mesh):
    return jax.shard_map(
        on_device,
        mesh=mesh,
        in_specs=(P("pix", "par"), P("parts", "pix")),
        out_specs=(P("parts", "par"), P("parts", "pix")),
        check_vma=False,
    )
```

```python
import functools

import jax
import jax.numpy as jnp
from jax import lax
from jax.experimental import pallas as pl
from jax.experimental.pallas import tpu as pltpu
from jax.sharding import PartitionSpec as P

GRID = 128
ITERS = 5
LANES = 128
EDGE = 2 * GRID
SLOTS = 8
TAIL = 16
BF16 = jnp.bfloat16
F32 = jnp.float32

GRAD_SQ, SMOOTH_SQ, CROSS = 0, 1, 2
IMAGE_SQ, BETA, GUESS = 2, 3, 4


def xor_pairs(count, offset):
    return [(i, i ^ offset) for i in range(count)]


def tree_sum(parts):
    while len(parts) > 1:
        parts = [parts[i] + parts[i + 1] for i in range(0, len(parts), 2)]
    return parts[0]


def lane_ids(sets):
    return lax.broadcasted_iota(jnp.int32, (sets, LANES), 1)


def beside(row):
    lane = lane_ids(row.shape[0])
    left = jnp.where(lane == 0, 0.0, pltpu.roll(row, 1, 1))
    right = jnp.where(lane == LANES - 1, 0.0, pltpu.roll(row, LANES - 1, 1))
    return left + right


def smooth_row(above, row, below):
    near = beside(row)
    if above is not None:
        near = near + above
    if below is not None:
        near = near + below
    return row - 0.25 * near


def lanes_of(columns, sets):
    lane = lane_ids(sets)
    block = jnp.zeros((sets, LANES), F32)
    for slot, column in columns.items():
        block = jnp.where(lane == slot, column, block)
    return block


def pack(block):
    block = jnp.where(lane_ids(block.shape[0]) < SLOTS, block, 0.0)
    high = block.astype(BF16).astype(F32)
    rest = block - high
    mid = rest.astype(BF16).astype(F32)
    low = (rest - mid).astype(BF16).astype(F32)
    return (high + pltpu.roll(mid, SLOTS, 1) + pltpu.roll(low, 2 * SLOTS, 1)).astype(BF16)


def unpack(packed):
    block = packed.astype(F32)
    mid = pltpu.roll(block, LANES - SLOTS, 1)
    low = pltpu.roll(block, LANES - 2 * SLOTS, 1)
    return jnp.where(lane_ids(block.shape[0]) < SLOTS, (block + mid) + low, 0.0)


def row_of(values, index):
    return values[:, index * GRID : (index + 1) * GRID]


def seam(lower, upper):
    low0, low1, up0, up1 = row_of(lower, 0), row_of(lower, 1), row_of(upper, 0), row_of(upper, 1)
    cross = smooth_row(low0, low1, None) * up0 + smooth_row(None, up0, up1) * low1
    return jnp.sum(0.0625 * (up0 * up0 + low1 * low1) - 0.5 * cross, axis=1, keepdims=True)


def merge(mine_ref, got_ref, above, below, pixels, step, final, tile):
    upper_side = (tile // step) % 2 == 1
    inside = tile % step
    scalar_at = pl.ds(pixels, LANES)
    if mine_ref.dtype == F32:
        mine, got = mine_ref[:, scalar_at], got_ref[:, scalar_at]
    else:
        mine, got = unpack(mine_ref[:, scalar_at]), unpack(got_ref[:, scalar_at])
    edges, got_edges = mine_ref[:, pixels + LANES :].astype(F32), got_ref[:, pixels + LANES :].astype(F32)
    if final:
        first = last = None
        lower_last = jnp.where(upper_side, got_edges, edges)
        upper_first = jnp.where(upper_side, edges, got_edges)
    else:
        first = jnp.where(upper_side, got_edges[:, :EDGE], edges[:, :EDGE])
        last = jnp.where(upper_side, edges[:, EDGE:], got_edges[:, EDGE:])
        lower_last = jnp.where(upper_side, got_edges[:, EDGE:], edges[:, EDGE:])
        upper_first = jnp.where(upper_side, edges[:, :EDGE], got_edges[:, :EDGE])
    sets = mine.shape[0]
    scalars = mine + got + lanes_of({SMOOTH_SQ: seam(lower_last, upper_first)}, sets)
    above = jnp.where(upper_side & (inside == 0), lower_last, above)
    below = jnp.where(jnp.logical_not(upper_side) & (inside == step - 1), upper_first, below)
    value = mine_ref[:, :pixels].astype(F32) + got_ref[:, :pixels].astype(F32)
    return value, scalars, first, last, above, below


def edge_columns(step, n_par):
    return EDGE if 2 * step >= n_par else 2 * EDGE


def store_edges(message, at, first, last, step, n_par, tile):
    if 2 * step >= n_par:
        edges = jnp.where((tile // step) % 2 == 1, first, last)
    else:
        edges = jnp.concatenate([first, last], axis=1)
    message[:, at:] = edges.astype(message.dtype)


def own_columns(offset, width):
    return pl.ds(pl.multiple_of((lax.axis_index("pix") ^ offset) * width, LANES), width)


def store_block(block, sent, scalar):
    sets, width = sent.shape
    for r in range(width // LANES):
        block[r * sets : (r + 1) * sets, :] = sent[:, r * LANES : (r + 1) * LANES]
    if scalar is not None:
        diagonal = lax.broadcasted_iota(jnp.int32, (sets, LANES), 0) == lane_ids(sets)
        row = jnp.sum(jnp.where(diagonal, scalar, 0.0), axis=0, keepdims=True)
        high = row.astype(BF16).astype(F32)
        mid = (row - high).astype(BF16).astype(F32)
        low = row - high - mid
        line = lax.broadcasted_iota(jnp.int32, (TAIL, LANES), 0)
        tail = jnp.where(line == 0, high, jnp.where(line == 1, mid, jnp.where(line == 2, low, 0.0)))
        block[sets * width // LANES :, :] = tail.astype(BF16)


def load_block(block, sets, width):
    rows = width // LANES
    return jnp.concatenate([block[r * sets : (r + 1) * sets, :].astype(F32) for r in range(rows)], axis=1)


def load_scalar(block, sets, width):
    tail = block[sets * width // LANES :, :].astype(F32)
    row = (tail[0:1] + tail[1:2]) + tail[2:3]
    diagonal = lax.broadcasted_iota(jnp.int32, (sets, LANES), 0) == lane_ids(sets)
    return jnp.sum(jnp.where(diagonal, row, 0.0), axis=1, keepdims=True)


def shard_kernel(offset, n_shards, first_sweep, closing, n_par, *refs):
    refs = list(refs)
    shard, green = refs.pop(0), refs.pop(0)
    twice = None if first_sweep else refs.pop(0)
    image_in = refs.pop(0) if offset else None
    sets, width = shard.shape
    pixels = green.shape[0]
    at = own_columns(offset, width) if n_shards > 1 else slice(None)
    value = shard[...]
    image = lax.dot_general(value, green[:, at], (((1,), (1,)), ((), ())), preferred_element_type=F32)
    if image_in is not None:
        image += image_in[...]
    rows = width // GRID
    grad_sq = jnp.zeros((sets, LANES), F32)
    smooth_sq = jnp.zeros((sets, LANES), F32)
    cross = jnp.zeros((sets, LANES), F32)
    wide = value.astype(F32)
    beside_it = None if first_sweep else twice[:, at]
    for r in range(rows):
        row = row_of(wide, r)
        alone = smooth_row(row_of(wide, r - 1) if r else None, row, row_of(wide, r + 1) if r + 1 < rows else None)
        grad_sq += row * row
        smooth_sq += alone * alone
        if not first_sweep:
            cross += row * row_of(beside_it, r)
    columns = {GRAD_SQ: jnp.sum(grad_sq, axis=1, keepdims=True), SMOOTH_SQ: jnp.sum(smooth_sq, axis=1, keepdims=True)}
    if not first_sweep:
        columns[CROSS] = jnp.sum(cross, axis=1, keepdims=True)
    scalars = lanes_of(columns, sets)
    if not closing:
        refs[0][...] = image
        refs[1][...] = scalars
        return
    others, other_scalars = refs[: n_shards - 1], refs[n_shards - 1 : 2 * n_shards - 2]
    whole, message = refs[2 * n_shards - 2 :]
    cells = whole.shape[1]
    order = [k for k in range(n_shards) if k != offset]
    found = {offset: scalars}
    if n_shards > 1:
        whole[:, at] = value
    else:
        whole[...] = value
    for k, other, other_scalar in zip(order, others, other_scalars):
        whole[:, own_columns(k, width)] = other[...]
        found[k] = other_scalar[...]
    total = tree_sum([found[k] for k in range(n_shards)])
    seams = jnp.zeros((sets, 1), F32)
    for k in range(1, n_shards):
        edge = k * width
        seams += seam(whole[:, edge - EDGE : edge].astype(F32), whole[:, edge : edge + EDGE].astype(F32))
    message[:, :pixels] = image
    message[:, pixels : pixels + LANES] = total + lanes_of({SMOOTH_SQ: seams}, sets)
    first, last = whole[:, :EDGE].astype(F32), whole[:, cells - EDGE :].astype(F32)
    store_edges(message, pixels + LANES, first, last, 1, n_par, lax.axis_index("par"))


def middle_kernel(step, n_par, *refs):
    if step == 1:
        mine, got, message, above, below = refs
        old_above = old_below = jnp.zeros(above.shape, F32)
    else:
        mine, got, above_in, below_in, message, above, below = refs
        old_above, old_below = above_in[...], below_in[...]
    pixels = mine.shape[1] - LANES - 2 * EDGE
    tile = lax.axis_index("par")
    value, scalars, first, last, up, down = merge(mine, got, old_above, old_below, pixels, step, False, tile)
    message[:, :pixels] = value.astype(BF16)
    message[:, pixels : pixels + LANES] = pack(scalars)
    store_edges(message, pixels + LANES, first, last, 2 * step, n_par, tile)
    above[...] = up
    below[...] = down


def image_kernel(step, n_pix, first_sweep, has_block, *refs):
    refs = list(refs)
    mine, got, above_in, below_in = (refs.pop(0) for _ in range(4))
    old_scalars, old_image = (None, None) if first_sweep else (refs.pop(0), refs.pop(0))
    green, lost = (refs.pop(0), refs.pop(0)) if has_block else (None, None)
    scalars, image, rounded, above, below = (refs.pop(0) for _ in range(5))
    sets, pixels = image.shape
    value, sums, _, _, up, down = merge(
        mine, got, above_in[...], below_in[...], pixels, step, True, lax.axis_index("par")
    )
    above[...] = up
    below[...] = down
    grad_sq = sums[:, GRAD_SQ : GRAD_SQ + 1]
    smooth_sq = sums[:, SMOOTH_SQ : SMOOTH_SQ + 1]
    beta = jnp.zeros((sets, 1), F32)
    if not first_sweep:
        beta = grad_sq / old_scalars[:, GRAD_SQ : GRAD_SQ + 1]
        old_smooth = old_scalars[:, SMOOTH_SQ : SMOOTH_SQ + 1]
        smooth_sq = smooth_sq + beta * (2.0 * sums[:, CROSS : CROSS + 1] + beta * old_smooth)
        value = value + beta * old_image[...]
    image[...] = value
    rounded[...] = value.astype(BF16)
    image_sq = jnp.zeros((sets, LANES), F32)
    for at in range(0, pixels, LANES):
        part = value[:, at : at + LANES]
        image_sq += part * part
    image_sq = jnp.sum(image_sq, axis=1, keepdims=True)
    guess = (n_pix * image_sq + smooth_sq) / grad_sq
    scalars[...] = lanes_of(
        {GRAD_SQ: grad_sq, SMOOTH_SQ: smooth_sq, IMAGE_SQ: image_sq, BETA: beta, GUESS: guess}, sets
    )
    if has_block:
        send_block(n_pix - 1, value.astype(BF16), green, lost, guess, image_sq, *refs)


def send_block(offset, image, green, lost, guess, image_sq, block, missed):
    part = jnp.dot(image, green[:, own_columns(offset, missed.shape[1])], preferred_element_type=F32)
    aimed = part if lost is None else part - guess * lost[...]
    sent = aimed.astype(BF16)
    store_block(block, sent, image_sq)
    missed[...] = part - sent.astype(F32)


def block_kernel(offset, rounded, scalars, green, lost, block, missed):
    guess, image_sq = scalars[:, GUESS : GUESS + 1], scalars[:, IMAGE_SQ : IMAGE_SQ + 1]
    send_block(offset, rounded[...], green, lost, guess, image_sq, block, missed)


def own_kernel(first_sweep, n_par, direct, has_product, *refs):
    refs = list(refs)
    scalars, above, below, whole = (refs.pop(0) for _ in range(4))
    old_direction = None if first_sweep else refs.pop(0)
    rounded, green = (refs.pop(0), refs.pop(0)) if has_product else (None, None)
    direction = refs.pop(0)
    cells = whole.shape[1]
    rows = cells // GRID
    if first_sweep:
        direction[:, :EDGE] = above[...]
        direction[:, EDGE : EDGE + cells] = whole[...].astype(F32)
        direction[:, EDGE + cells :] = below[...]
    else:
        beta = scalars[:, BETA : BETA + 1]
        direction[:, :EDGE] = above[...] + beta * old_direction[:, :EDGE]
        direction[:, EDGE : EDGE + cells] = whole[...].astype(F32) + beta * old_direction[:, EDGE : EDGE + cells]
        direction[:, EDGE + cells :] = below[...] + beta * old_direction[:, EDGE + cells :]
    if not has_product:
        return
    twice, own, once = refs
    tile = lax.axis_index("par")

    def from_ref(ref, r):
        return ref[:, r * GRID : (r + 1) * GRID]

    for r in range(rows + 2):
        row = smooth_row(from_ref(direction, r), from_ref(direction, r + 1), from_ref(direction, r + 2))
        if r == 0:
            row = jnp.where(tile == 0, 0.0, row)
        if r == rows + 1:
            row = jnp.where(tile == n_par - 1, 0.0, row)
        once[:, r * GRID : (r + 1) * GRID] = row
    for r in range(rows):
        row = smooth_row(from_ref(once, r), from_ref(once, r + 1), from_ref(once, r + 2))
        twice[:, r * GRID : (r + 1) * GRID] = row
    if direct:
        at = own_columns(0, own.shape[1])
        own[...] = jnp.dot(rounded[...], green[:, at], preferred_element_type=F32) + twice[:, at]
    else:
        own[...] = jnp.dot(rounded[...], green[...], preferred_element_type=F32)


def start_kernel(observed, green, own, *refs):
    count = len(refs) // 2
    image = observed[...]
    for offset in range(count, 0, -1):
        send_block(offset, image, green, None, None, None, refs[offset - 1], refs[count + offset - 1])
    own[...] = jnp.dot(image, green[:, own_columns(0, own.shape[1])], preferred_element_type=F32)


def receive_start_kernel(own, *refs):
    got, (grad, rounded) = refs[:-2][::-1], refs[-2:]
    sets, width = own.shape
    value = tree_sum([own[...]] + [load_block(ref, sets, width) for ref in got])
    grad[...] = value
    rounded[...] = value.astype(BF16)


def step_length(scalars, others):
    image_sq = tree_sum([scalars[:, IMAGE_SQ : IMAGE_SQ + 1]] + others)
    return scalars[:, GRAD_SQ : GRAD_SQ + 1] / (image_sq + scalars[:, SMOOTH_SQ : SMOOTH_SQ + 1])


def receive_kernel(own, scalars, old_grad, *refs):
    got, (grad, rounded, length) = refs[:-3][::-1], refs[-3:]
    sets, width = own.shape
    step_len = step_length(scalars, [load_scalar(ref, sets, width) for ref in got])
    change = tree_sum([own[...]] + [load_block(ref, sets, width) for ref in got])
    value = old_grad[...] - step_len * change
    grad[...] = value
    rounded[...] = value.astype(BF16)
    length[...] = jnp.broadcast_to(step_len, length.shape)


def update_kernel(count, length, direction, image, solution, residual, *refs):
    step_len = length[:, :1]
    lost, missed = refs[:count], refs[count : 2 * count]
    new_solution, new_residual = refs[2 * count : 2 * count + 2]
    for old, change, new in zip(lost, missed, refs[2 * count + 2 :]):
        new[...] = old[...] - step_len * change[...]
    cells = solution.shape[1]
    new_solution[...] = solution[...] + step_len * direction[:, EDGE : EDGE + cells]
    new_residual[...] = residual[...] - step_len * image[...]


def finish_kernel(scalars, *refs):
    got, (direction, image, solution, residual, new_solution, new_residual) = refs[:-6][::-1], refs[-6:]
    step_len = step_length(scalars, [ref[:, IMAGE_SQ : IMAGE_SQ + 1] for ref in got])
    cells = solution.shape[1]
    new_solution[...] = solution[...] + step_len * direction[:, EDGE : EDGE + cells]
    new_residual[...] = residual[...] - step_len * image[...]


def call(kernel, operands, outs, scratch=(), flops=0, limit=24 << 20):
    vmem = pl.BlockSpec(memory_space=pltpu.VMEM)
    shapes = [jax.ShapeDtypeStruct(*out) for out in outs]
    moved = sum(x.size * x.dtype.itemsize for x in [*operands, *shapes])
    return pl.pallas_call(
        kernel,
        in_specs=[vmem] * len(operands),
        out_specs=[vmem] * len(outs),
        out_shape=shapes,
        scratch_shapes=list(scratch),
        name=getattr(kernel, "func", kernel).__name__,
        compiler_params=pltpu.CompilerParams(vmem_limit_bytes=limit),
        cost_estimate=pl.CostEstimate(flops=flops or moved, bytes_accessed=moved, transcendentals=0),
    )(*operands)


def exchange(blocks, axis, count):
    got = [lax.ppermute(blocks[k - 1], axis, xor_pairs(count, k)) for k in range(count - 1, 0, -1)]
    return got[::-1]


def on_device(green, observed):
    sets = observed.shape[0]
    pixels, cells = green.shape
    n_pix, n_par = lax.axis_size("pix"), lax.axis_size("par")
    here = lax.axis_index("pix")
    width = cells // n_pix
    direct = n_pix <= 8 and width % LANES == 0
    flops = 2 * sets * pixels * cells
    part_flops = flops // n_pix
    count = n_pix - 1 if direct else 0
    shard, rounded_shard = ((sets, width), F32), ((sets, width), BF16)
    plain = ((sets * width // LANES, LANES), BF16)
    block = ((sets * width // LANES + TAIL, LANES), BF16)
    scalar = ((sets, LANES), F32)
    line, wide, edge = ((sets, pixels), F32), ((sets, cells), F32), ((sets, EDGE), F32)
    ring = ((sets, cells + 2 * EDGE), F32)

    lost = []
    if direct:
        own, *rest = call(start_kernel, [observed, green], [shard] + [plain] * count + [shard] * count, flops=flops)
        blocks, lost = rest[:count], rest[count:]
        got = exchange(blocks, "pix", n_pix)
    else:
        partial = jnp.dot(observed, green, preferred_element_type=F32)
        own, got = lax.psum_scatter(partial, "pix", scatter_dimension=1, tiled=True), []
    grad, rounded_grad = call(receive_start_kernel, [own, *got[::-1]], [shard, rounded_shard])
    solution = jnp.zeros((sets, cells), F32)
    residual = observed.astype(F32)
    scalars = image = direction = twice = None
    for sweep in range(ITERS):
        first, final = sweep == 0, sweep + 1 == ITERS
        if direct:
            shards = [rounded_grad] + exchange([rounded_grad] * count, "pix", n_pix)
        else:
            shards = [lax.all_gather(rounded_grad, "pix", axis=1, tiled=True)]
        beside_them = [] if first else [twice]

        def message_of(step):
            return ((sets, pixels + LANES + edge_columns(step, n_par)), F32 if step == 1 else BF16)

        order = [0] + list(range(len(shards) - 1, 0, -1))
        partial, parts = [], {}
        for k in order[:-1]:
            kernel = functools.partial(shard_kernel, k, len(shards), first, False, n_par)
            out, parts[k] = call(kernel, [shards[k], green, *beside_them, *partial], [line, scalar], flops=part_flops)
            partial = [out]
        k = order[-1]
        others = sorted(parts)
        whole, message = call(
            functools.partial(shard_kernel, k, len(shards), first, True, n_par),
            [shards[k], green, *beside_them, *partial]
            + [shards[o] for o in others]
            + [parts[o] for o in others],
            [((sets, cells), BF16), message_of(1)],
            flops=part_flops,
        )
        step, above, below = 1, None, None
        while True:
            got = lax.ppermute(message, "par", xor_pairs(n_par, step))
            if 2 * step >= n_par:
                break
            message, above, below = call(
                functools.partial(middle_kernel, step, n_par),
                [message, got, *([] if step == 1 else [above, below])],
                [message_of(2 * step), edge, edge],
            )
            step *= 2
        if above is None:
            above = below = jnp.zeros(edge[0], F32)
        has_block = direct and not final
        missed = [None] * count
        blocks = [None] * count
        scalars, image, rounded, above, below, *rest = call(
            functools.partial(image_kernel, step, n_pix, first, has_block),
            [message, got, above, below]
            + ([] if first else [scalars, image])
            + ([green, lost[-1]] if has_block else []),
            [scalar, line, ((sets, pixels), BF16), edge, edge] + ([block, shard] if has_block else []),
            flops=part_flops if has_block else 0,
        )
        olds = [] if first else [direction]
        if final:
            (direction,) = call(
                functools.partial(own_kernel, first, n_par, direct, False),
                [scalars, above, below, whole, *olds],
                [ring],
            )
            if direct:
                got = exchange([scalars] * count, "pix", n_pix)
            else:
                got = []
                scalars = scalars.at[:, IMAGE_SQ].set(lax.psum(scalars[:, IMAGE_SQ], "pix"))
            return tuple(call(finish_kernel, [scalars, *got[::-1], direction, image, solution, residual], [wide, line]))
        if direct:
            blocks[-1], missed[-1] = rest
            for k in range(count - 1, 0, -1):
                blocks[k - 1], missed[k - 1] = call(
                    functools.partial(block_kernel, k),
                    [rounded, scalars, green, lost[k - 1]],
                    [block, shard],
                    flops=part_flops,
                )
        direction, twice, own = call(
            functools.partial(own_kernel, first, n_par, direct, True),
            [scalars, above, below, whole, *olds, rounded, green],
            [ring, wide, shard if direct else wide],
            [pltpu.VMEM((sets, cells + EDGE), F32)],
            part_flops if direct else flops,
        )
        if direct:
            got = exchange(blocks, "pix", n_pix)
        else:
            got = []
            own = lax.psum_scatter(own, "pix", scatter_dimension=1, tiled=True)
            own = own + lax.dynamic_slice_in_dim(twice, here * width, width, axis=1)
            scalars = scalars.at[:, IMAGE_SQ].set(lax.psum(scalars[:, IMAGE_SQ], "pix"))
        grad, rounded_grad, length = call(
            receive_kernel, [own, scalars, grad, *got[::-1]], [shard, rounded_shard, scalar]
        )
        solution, residual, *lost = call(
            functools.partial(update_kernel, count),
            [length, direction, image, solution, residual, *lost, *missed],
            [wide, line] + [shard] * count,
        )


def solution(mesh):
    return jax.shard_map(
        on_device,
        mesh=mesh,
        in_specs=(P("pix", "par"), P("parts", "pix")),
        out_specs=(P("parts", "par"), P("parts", "pix")),
        check_vma=False,
    )
```

```python
import functools
import math

import jax
import jax.numpy as jnp
from jax import lax
from jax.experimental import pallas as pl
from jax.experimental.pallas import tpu as pltpu
from jax.sharding import PartitionSpec as P

GRID = 128
ITERS = 5
LANES = 128
EDGE = 2 * GRID
SLOTS = 8
TAIL = 16
BF16 = jnp.bfloat16
F32 = jnp.float32

GRAD_SQ, SMOOTH_SQ, CROSS = 0, 1, 2
IMAGE_SQ, BETA, GUESS = 2, 3, 4


def xor_pairs(count, offset):
    return [(i, i ^ offset) for i in range(count)]


def send_order(count):
    return [count - 1] + list(range(1, count - 1))


def tree_sum(parts):
    while len(parts) > 1:
        parts = [parts[i] + parts[i + 1] for i in range(0, len(parts), 2)]
    return parts[0]


def lane_ids(sets):
    return lax.broadcasted_iota(jnp.int32, (sets, LANES), 1)


def beside(row):
    lane = lane_ids(row.shape[0])
    left = jnp.where(lane == 0, 0.0, pltpu.roll(row, 1, 1))
    right = jnp.where(lane == LANES - 1, 0.0, pltpu.roll(row, LANES - 1, 1))
    return left + right


def smooth_row(above, row, below):
    near = beside(row)
    if above is not None:
        near = near + above
    if below is not None:
        near = near + below
    return row - 0.25 * near


def lanes_of(columns, sets):
    lane = lane_ids(sets)
    block = jnp.zeros((sets, LANES), F32)
    for slot, column in columns.items():
        block = jnp.where(lane == slot, column, block)
    return block


def pack(block):
    block = jnp.where(lane_ids(block.shape[0]) < SLOTS, block, 0.0)
    high = block.astype(BF16).astype(F32)
    rest = block - high
    mid = rest.astype(BF16).astype(F32)
    low = (rest - mid).astype(BF16).astype(F32)
    return (high + pltpu.roll(mid, SLOTS, 1) + pltpu.roll(low, 2 * SLOTS, 1)).astype(BF16)


def unpack(packed):
    block = packed.astype(F32)
    mid = pltpu.roll(block, LANES - SLOTS, 1)
    low = pltpu.roll(block, LANES - 2 * SLOTS, 1)
    return jnp.where(lane_ids(block.shape[0]) < SLOTS, (block + mid) + low, 0.0)


def row_of(values, index):
    return values[:, index * GRID : (index + 1) * GRID]


def seam(lower, upper):
    low0, low1, up0, up1 = row_of(lower, 0), row_of(lower, 1), row_of(upper, 0), row_of(upper, 1)
    cross = smooth_row(low0, low1, None) * up0 + smooth_row(None, up0, up1) * low1
    return jnp.sum(0.0625 * (up0 * up0 + low1 * low1) - 0.5 * cross, axis=1, keepdims=True)


def merge(mine_ref, got_ref, above, below, pixels, step, final, tile):
    upper_side = (tile // step) % 2 == 1
    inside = tile % step
    scalar_at = pl.ds(pixels, LANES)
    if mine_ref.dtype == F32:
        mine, got = mine_ref[:, scalar_at], got_ref[:, scalar_at]
    else:
        mine, got = unpack(mine_ref[:, scalar_at]), unpack(got_ref[:, scalar_at])
    edges, got_edges = mine_ref[:, pixels + LANES :].astype(F32), got_ref[:, pixels + LANES :].astype(F32)
    if final:
        first = last = None
        lower_last = jnp.where(upper_side, got_edges, edges)
        upper_first = jnp.where(upper_side, edges, got_edges)
    else:
        first = jnp.where(upper_side, got_edges[:, :EDGE], edges[:, :EDGE])
        last = jnp.where(upper_side, edges[:, EDGE:], got_edges[:, EDGE:])
        lower_last = jnp.where(upper_side, got_edges[:, EDGE:], edges[:, EDGE:])
        upper_first = jnp.where(upper_side, edges[:, :EDGE], got_edges[:, :EDGE])
    sets = mine.shape[0]
    scalars = mine + got + lanes_of({SMOOTH_SQ: seam(lower_last, upper_first)}, sets)
    above = jnp.where(upper_side & (inside == 0), lower_last, above)
    below = jnp.where(jnp.logical_not(upper_side) & (inside == step - 1), upper_first, below)
    value = mine_ref[:, :pixels].astype(F32) + got_ref[:, :pixels].astype(F32)
    return value, scalars, first, last, above, below


def edge_columns(step, n_par):
    return EDGE if 2 * step >= n_par else 2 * EDGE


def store_edges(message, at, first, last, step, n_par, tile):
    if 2 * step >= n_par:
        edges = jnp.where((tile // step) % 2 == 1, first, last)
    else:
        edges = jnp.concatenate([first, last], axis=1)
    message[:, at:] = edges.astype(message.dtype)


def own_columns(offset, width):
    return pl.ds(pl.multiple_of((lax.axis_index("pix") ^ offset) * width, LANES), width)


def store_block(block, sent, scalar):
    sets, width = sent.shape
    for r in range(width // LANES):
        block[r * sets : (r + 1) * sets, :] = sent[:, r * LANES : (r + 1) * LANES]
    if scalar is not None:
        diagonal = lax.broadcasted_iota(jnp.int32, (sets, LANES), 0) == lane_ids(sets)
        row = jnp.sum(jnp.where(diagonal, scalar, 0.0), axis=0, keepdims=True)
        high = row.astype(BF16).astype(F32)
        mid = (row - high).astype(BF16).astype(F32)
        low = row - high - mid
        line = lax.broadcasted_iota(jnp.int32, (TAIL, LANES), 0)
        tail = jnp.where(line == 0, high, jnp.where(line == 1, mid, jnp.where(line == 2, low, 0.0)))
        block[sets * width // LANES :, :] = tail.astype(BF16)


def load_block(block, sets, width):
    rows = width // LANES
    return jnp.concatenate([block[r * sets : (r + 1) * sets, :].astype(F32) for r in range(rows)], axis=1)


def load_scalar(block, sets, width):
    tail = block[sets * width // LANES :, :].astype(F32)
    row = (tail[0:1] + tail[1:2]) + tail[2:3]
    diagonal = lax.broadcasted_iota(jnp.int32, (sets, LANES), 0) == lane_ids(sets)
    return jnp.sum(jnp.where(diagonal, row, 0.0), axis=1, keepdims=True)


def shard_kernel(offset, n_shards, first_sweep, closing, n_par, *refs):
    refs = list(refs)
    shard, green = refs.pop(0), refs.pop(0)
    twice = None if first_sweep else refs.pop(0)
    image_in = refs.pop(0) if offset else None
    sets, width = shard.shape
    pixels = green.shape[0]
    at = own_columns(offset, width) if n_shards > 1 else slice(None)
    value = shard[...]
    image = lax.dot_general(value, green[:, at], (((1,), (1,)), ((), ())), preferred_element_type=F32)
    if image_in is not None:
        image += image_in[...]
    rows = width // GRID
    grad_sq = jnp.zeros((sets, LANES), F32)
    smooth_sq = jnp.zeros((sets, LANES), F32)
    cross = jnp.zeros((sets, LANES), F32)
    wide = value.astype(F32)
    beside_it = None if first_sweep else twice[:, at]
    for r in range(rows):
        row = row_of(wide, r)
        alone = smooth_row(row_of(wide, r - 1) if r else None, row, row_of(wide, r + 1) if r + 1 < rows else None)
        grad_sq += row * row
        smooth_sq += alone * alone
        if not first_sweep:
            cross += row * row_of(beside_it, r)
    columns = {GRAD_SQ: jnp.sum(grad_sq, axis=1, keepdims=True), SMOOTH_SQ: jnp.sum(smooth_sq, axis=1, keepdims=True)}
    if not first_sweep:
        columns[CROSS] = jnp.sum(cross, axis=1, keepdims=True)
    scalars = lanes_of(columns, sets)
    if not closing:
        refs[0][...] = image
        refs[1][...] = scalars
        return
    others, other_scalars = refs[: n_shards - 1], refs[n_shards - 1 : 2 * n_shards - 2]
    whole, message = refs[2 * n_shards - 2 :]
    cells = whole.shape[1]
    order = [k for k in range(n_shards) if k != offset]
    found = {offset: scalars}
    if n_shards > 1:
        whole[:, at] = value
    else:
        whole[...] = value
    for k, other, other_scalar in zip(order, others, other_scalars):
        whole[:, own_columns(k, width)] = other[...]
        found[k] = other_scalar[...]
    total = tree_sum([found[k] for k in range(n_shards)])
    seams = jnp.zeros((sets, 1), F32)
    for k in range(1, n_shards):
        edge = k * width
        seams += seam(whole[:, edge - EDGE : edge].astype(F32), whole[:, edge : edge + EDGE].astype(F32))
    message[:, :pixels] = image
    message[:, pixels : pixels + LANES] = total + lanes_of({SMOOTH_SQ: seams}, sets)
    first, last = whole[:, :EDGE].astype(F32), whole[:, cells - EDGE :].astype(F32)
    store_edges(message, pixels + LANES, first, last, 1, n_par, lax.axis_index("par"))


def middle_kernel(step, n_par, *refs):
    if step == 1:
        mine, got, message, above, below = refs
        old_above = old_below = jnp.zeros(above.shape, F32)
    else:
        mine, got, above_in, below_in, message, above, below = refs
        old_above, old_below = above_in[...], below_in[...]
    pixels = mine.shape[1] - LANES - 2 * EDGE
    tile = lax.axis_index("par")
    value, scalars, first, last, up, down = merge(mine, got, old_above, old_below, pixels, step, False, tile)
    message[:, :pixels] = value.astype(BF16)
    message[:, pixels : pixels + LANES] = pack(scalars)
    store_edges(message, pixels + LANES, first, last, 2 * step, n_par, tile)
    above[...] = up
    below[...] = down


def image_kernel(step, n_pix, first_sweep, has_block, *refs):
    refs = list(refs)
    mine, got, above_in, below_in = (refs.pop(0) for _ in range(4))
    old_scalars, old_image = (None, None) if first_sweep else (refs.pop(0), refs.pop(0))
    green, lost = (refs.pop(0), refs.pop(0)) if has_block else (None, None)
    scalars, image, rounded, above, below = (refs.pop(0) for _ in range(5))
    sets, pixels = image.shape
    value, sums, _, _, up, down = merge(
        mine, got, above_in[...], below_in[...], pixels, step, True, lax.axis_index("par")
    )
    above[...] = up
    below[...] = down
    grad_sq = sums[:, GRAD_SQ : GRAD_SQ + 1]
    smooth_sq = sums[:, SMOOTH_SQ : SMOOTH_SQ + 1]
    beta = jnp.zeros((sets, 1), F32)
    if not first_sweep:
        beta = grad_sq / old_scalars[:, GRAD_SQ : GRAD_SQ + 1]
        old_smooth = old_scalars[:, SMOOTH_SQ : SMOOTH_SQ + 1]
        smooth_sq = smooth_sq + beta * (2.0 * sums[:, CROSS : CROSS + 1] + beta * old_smooth)
        value = value + beta * old_image[...]
    image[...] = value
    rounded[...] = value.astype(BF16)
    image_sq = jnp.zeros((sets, LANES), F32)
    for at in range(0, pixels, LANES):
        part = value[:, at : at + LANES]
        image_sq += part * part
    image_sq = jnp.sum(image_sq, axis=1, keepdims=True)
    guess = (n_pix * image_sq + smooth_sq) / grad_sq
    scalars[...] = lanes_of(
        {GRAD_SQ: grad_sq, SMOOTH_SQ: smooth_sq, IMAGE_SQ: image_sq, BETA: beta, GUESS: guess}, sets
    )
    if has_block:
        send_block(send_order(n_pix)[0], value.astype(BF16), green, lost, guess, image_sq, *refs)


def send_block(offset, image, green, lost, guess, image_sq, block, missed):
    part = jnp.dot(image, green[:, own_columns(offset, missed.shape[1])], preferred_element_type=F32)
    aimed = part if lost is None else part - guess * lost[...]
    sent = aimed.astype(BF16)
    store_block(block, sent, image_sq)
    missed[...] = part - sent.astype(F32)


def block_kernel(offset, rounded, scalars, green, lost, block, missed):
    guess, image_sq = scalars[:, GUESS : GUESS + 1], scalars[:, IMAGE_SQ : IMAGE_SQ + 1]
    send_block(offset, rounded[...], green, lost, guess, image_sq, block, missed)


def own_kernel(first_sweep, n_par, direct, has_product, *refs):
    refs = list(refs)
    scalars, above, below, whole = (refs.pop(0) for _ in range(4))
    old_direction = None if first_sweep else refs.pop(0)
    rounded, green = (refs.pop(0), refs.pop(0)) if has_product else (None, None)
    direction = refs.pop(0)
    cells = whole.shape[1]
    rows = cells // GRID
    if first_sweep:
        direction[:, :EDGE] = above[...]
        direction[:, EDGE : EDGE + cells] = whole[...].astype(F32)
        direction[:, EDGE + cells :] = below[...]
    else:
        beta = scalars[:, BETA : BETA + 1]
        direction[:, :EDGE] = above[...] + beta * old_direction[:, :EDGE]
        direction[:, EDGE : EDGE + cells] = whole[...].astype(F32) + beta * old_direction[:, EDGE : EDGE + cells]
        direction[:, EDGE + cells :] = below[...] + beta * old_direction[:, EDGE + cells :]
    if not has_product:
        return
    twice, own, once = refs
    tile = lax.axis_index("par")

    def from_ref(ref, r):
        return ref[:, r * GRID : (r + 1) * GRID]

    for r in range(rows + 2):
        row = smooth_row(from_ref(direction, r), from_ref(direction, r + 1), from_ref(direction, r + 2))
        if r == 0:
            row = jnp.where(tile == 0, 0.0, row)
        if r == rows + 1:
            row = jnp.where(tile == n_par - 1, 0.0, row)
        once[:, r * GRID : (r + 1) * GRID] = row
    for r in range(rows):
        row = smooth_row(from_ref(once, r), from_ref(once, r + 1), from_ref(once, r + 2))
        twice[:, r * GRID : (r + 1) * GRID] = row
    if direct:
        at = own_columns(0, own.shape[1])
        own[...] = jnp.dot(rounded[...], green[:, at], preferred_element_type=F32) + twice[:, at]
    else:
        own[...] = jnp.dot(rounded[...], green[...], preferred_element_type=F32)


def start_kernel(observed_at, green_at, green, own, *refs):
    refs, (observed, observed_sem, sems) = refs[:-3], refs[-3:]
    n_pix = len(refs) // 2 + 1
    width = own.shape[1]
    order = send_order(n_pix) + [0]
    first = pltpu.make_async_copy(observed_at, observed, observed_sem)
    first.start()
    copies = []
    for i, offset in enumerate(order):
        at = own_columns(offset, width)
        copies.append(pltpu.make_async_copy(green_at.at[:, at], green.at[:, at], sems.at[i]))
        copies[-1].start()
    first.wait()
    image = observed[...]
    for i, offset in enumerate(order):
        copies[i].wait()
        if offset:
            send_block(offset, image, green, None, None, None, refs[i], refs[n_pix - 1 + i])
        else:
            own[...] = jnp.dot(image, green[:, own_columns(0, width)], preferred_element_type=F32)


def receive_start_kernel(own, *refs):
    got, (grad, rounded) = refs[:-2], refs[-2:]
    sets, width = own.shape
    count = len(got) + 1
    value = tree_sum(by_offset(count, own[...], [load_block(ref, sets, width) for ref in got]))
    grad[...] = value
    rounded[...] = value.astype(BF16)


def step_length(scalars, others):
    own = scalars[:, IMAGE_SQ : IMAGE_SQ + 1]
    image_sq = tree_sum(by_offset(len(others) + 1, own, others))
    return scalars[:, GRAD_SQ : GRAD_SQ + 1] / (image_sq + scalars[:, SMOOTH_SQ : SMOOTH_SQ + 1])


def receive_kernel(own, scalars, old_grad, *refs):
    got, (grad, rounded, length) = refs[:-3], refs[-3:]
    sets, width = own.shape
    step_len = step_length(scalars, [load_scalar(ref, sets, width) for ref in got])
    change = tree_sum(by_offset(len(got) + 1, own[...], [load_block(ref, sets, width) for ref in got]))
    value = old_grad[...] - step_len * change
    grad[...] = value
    rounded[...] = value.astype(BF16)
    length[...] = jnp.broadcast_to(step_len, length.shape)


def update_kernel(count, length, direction, image, solution, residual, *refs):
    step_len = length[:, :1]
    lost, missed = refs[:count], refs[count : 2 * count]
    new_solution, new_residual = refs[2 * count : 2 * count + 2]
    for old, change, new in zip(lost, missed, refs[2 * count + 2 :]):
        new[...] = old[...] - step_len * change[...]
    cells = solution.shape[1]
    new_solution[...] = solution[...] + step_len * direction[:, EDGE : EDGE + cells]
    new_residual[...] = residual[...] - step_len * image[...]


def finish_kernel(scalars, *refs):
    got, (direction, image, solution, residual, new_solution, new_residual) = refs[:-6], refs[-6:]
    step_len = step_length(scalars, [ref[:, IMAGE_SQ : IMAGE_SQ + 1] for ref in got])
    cells = solution.shape[1]
    new_solution[...] = solution[...] + step_len * direction[:, EDGE : EDGE + cells]
    new_residual[...] = residual[...] - step_len * image[...]


def call(kernel, operands, outs, scratch=(), flops=0, limit=24 << 20, space=pltpu.VMEM):
    vmem = pl.BlockSpec(memory_space=pltpu.VMEM)
    shapes = [jax.ShapeDtypeStruct(*out) if isinstance(out, tuple) else out for out in outs]
    moved = sum(math.prod(x.shape) * jnp.dtype(x.dtype).itemsize for x in [*operands, *shapes])
    return pl.pallas_call(
        kernel,
        in_specs=[pl.BlockSpec(memory_space=space)] * len(operands),
        out_specs=[vmem] * len(outs),
        out_shape=shapes,
        scratch_shapes=list(scratch),
        name=getattr(kernel, "func", kernel).__name__,
        compiler_params=pltpu.CompilerParams(vmem_limit_bytes=limit),
        cost_estimate=pl.CostEstimate(flops=flops or moved, bytes_accessed=moved, transcendentals=0),
    )(*operands)


def exchange(blocks, axis, count):
    return {k: lax.ppermute(blocks[k], axis, xor_pairs(count, k)) for k in send_order(count)}


def by_offset(count, own, got):
    found = {0: own, **dict(zip(send_order(count), got))}
    return [found[k] for k in range(count)]


def on_device(green, observed):
    sets = observed.shape[0]
    pixels, cells = green.shape
    n_pix, n_par = lax.axis_size("pix"), lax.axis_size("par")
    here = lax.axis_index("pix")
    width = cells // n_pix
    direct = n_pix <= 8 and width % LANES == 0
    flops = 2 * sets * pixels * cells
    part_flops = flops // n_pix
    count = n_pix - 1 if direct else 0
    shard, rounded_shard = ((sets, width), F32), ((sets, width), BF16)
    plain = ((sets * width // LANES, LANES), BF16)
    block = ((sets * width // LANES + TAIL, LANES), BF16)
    scalar = ((sets, LANES), F32)
    line, wide, edge = ((sets, pixels), F32), ((sets, cells), F32), ((sets, EDGE), F32)
    ring = ((sets, cells + 2 * EDGE), F32)

    order = send_order(n_pix) if direct else []
    lost, got = {}, {}
    if direct:
        green, own, *rest = call(
            start_kernel,
            [observed, green],
            [pltpu.VMEM(*out) for out in [(green.shape, BF16), shard] + [plain] * count + [shard] * count],
            [pltpu.VMEM(observed.shape, BF16), pltpu.SemaphoreType.DMA, pltpu.SemaphoreType.DMA((n_pix,))],
            flops,
            limit=48 << 20,
            space=pltpu.HBM,
        )
        lost = dict(zip(order, rest[count:]))
        got = exchange(dict(zip(order, rest)), "pix", n_pix)
    else:
        partial = jnp.dot(observed, green, preferred_element_type=F32)
        own = lax.psum_scatter(partial, "pix", scatter_dimension=1, tiled=True)
    grad, rounded_grad = call(receive_start_kernel, [own, *got.values()], [shard, rounded_shard])
    solution = jnp.zeros((sets, cells), F32)
    residual = observed.astype(F32)
    scalars = image = direction = twice = None
    for sweep in range(ITERS):
        first, final = sweep == 0, sweep + 1 == ITERS
        if direct:
            shards = {0: rounded_grad, **exchange(dict.fromkeys(order, rounded_grad), "pix", n_pix)}
        else:
            shards = {0: lax.all_gather(rounded_grad, "pix", axis=1, tiled=True)}
        beside_them = [] if first else [twice]

        def message_of(step):
            return ((sets, pixels + LANES + edge_columns(step, n_par)), F32 if step == 1 else BF16)

        partial, parts = [], {}
        closing = ([0] + order)[-1]
        for k in ([0] + order)[:-1]:
            kernel = functools.partial(shard_kernel, k, len(shards), first, False, n_par)
            out, parts[k] = call(kernel, [shards[k], green, *beside_them, *partial], [line, scalar], flops=part_flops)
            partial = [out]
        others = sorted(parts)
        whole, message = call(
            functools.partial(shard_kernel, closing, len(shards), first, True, n_par),
            [shards[closing], green, *beside_them, *partial]
            + [shards[o] for o in others]
            + [parts[o] for o in others],
            [((sets, cells), BF16), message_of(1)],
            flops=part_flops,
        )
        step, above, below = 1, None, None
        while True:
            got = lax.ppermute(message, "par", xor_pairs(n_par, step))
            if 2 * step >= n_par:
                break
            message, above, below = call(
                functools.partial(middle_kernel, step, n_par),
                [message, got, *([] if step == 1 else [above, below])],
                [message_of(2 * step), edge, edge],
            )
            step *= 2
        if above is None:
            above = below = jnp.zeros(edge[0], F32)
        has_block = direct and not final
        blocks, missed = {}, {}
        scalars, image, rounded, above, below, *rest = call(
            functools.partial(image_kernel, step, n_pix, first, has_block),
            [message, got, above, below]
            + ([] if first else [scalars, image])
            + ([green, lost[order[0]]] if has_block else []),
            [scalar, line, ((sets, pixels), BF16), edge, edge] + ([block, shard] if has_block else []),
            flops=part_flops if has_block else 0,
        )
        olds = [] if first else [direction]
        if final:
            (direction,) = call(
                functools.partial(own_kernel, first, n_par, direct, False),
                [scalars, above, below, whole, *olds],
                [ring],
            )
            if direct:
                got = exchange(dict.fromkeys(order, scalars), "pix", n_pix)
            else:
                got = {}
                scalars = scalars.at[:, IMAGE_SQ].set(lax.psum(scalars[:, IMAGE_SQ], "pix"))
            return tuple(call(finish_kernel, [scalars, *got.values(), direction, image, solution, residual], [wide, line]))
        if direct:
            blocks[order[0]], missed[order[0]] = rest
            for k in order[1:]:
                blocks[k], missed[k] = call(
                    functools.partial(block_kernel, k),
                    [rounded, scalars, green, lost[k]],
                    [block, shard],
                    flops=part_flops,
                )
        direction, twice, own = call(
            functools.partial(own_kernel, first, n_par, direct, True),
            [scalars, above, below, whole, *olds, rounded, green],
            [ring, wide, shard if direct else wide],
            [pltpu.VMEM((sets, cells + EDGE), F32)],
            part_flops if direct else flops,
        )
        if direct:
            got = exchange(blocks, "pix", n_pix)
        else:
            got = {}
            own = lax.psum_scatter(own, "pix", scatter_dimension=1, tiled=True)
            own = own + lax.dynamic_slice_in_dim(twice, here * width, width, axis=1)
            scalars = scalars.at[:, IMAGE_SQ].set(lax.psum(scalars[:, IMAGE_SQ], "pix"))
        grad, rounded_grad, length = call(
            receive_kernel, [own, scalars, grad, *got.values()], [shard, rounded_shard, scalar]
        )
        solution, residual, *rest = call(
            functools.partial(update_kernel, count),
            [length, direction, image, solution, residual, *lost.values(), *missed.values()],
            [wide, line] + [shard] * count,
        )
        lost = dict(zip(order, rest))


def solution(mesh):
    return jax.shard_map(
        on_device,
        mesh=mesh,
        in_specs=(P("pix", "par"), P("parts", "pix")),
        out_specs=(P("parts", "par"), P("parts", "pix")),
        check_vma=False,
    )
```

```python
import functools
import math

import jax
import jax.numpy as jnp
from jax import lax
from jax.experimental import pallas as pl
from jax.experimental.pallas import tpu as pltpu
from jax.sharding import PartitionSpec as P

GRID = 128
ITERS = 5
LANES = 128
EDGE = 2 * GRID
SLOTS = 8
TAIL = 8
BF16 = jnp.bfloat16
F32 = jnp.float32

GRAD_SQ, SMOOTH_SQ, CROSS = 0, 1, 2
IMAGE_SQ, BETA, GUESS = 2, 3, 4


def xor_pairs(count, offset):
    return [(i, i ^ offset) for i in range(count)]


def send_order(count):
    return [count - 1] + list(range(1, count - 1))


def gather_order(count):
    return [count - 1] + list(range(1, count - 1))


def tree_sum(parts):
    while len(parts) > 1:
        parts = [parts[i] + parts[i + 1] for i in range(0, len(parts), 2)]
    return parts[0]


def lane_ids(sets):
    return lax.broadcasted_iota(jnp.int32, (sets, LANES), 1)


def beside(row):
    lane = lane_ids(row.shape[0])
    left = jnp.where(lane == 0, 0.0, pltpu.roll(row, 1, 1))
    right = jnp.where(lane == LANES - 1, 0.0, pltpu.roll(row, LANES - 1, 1))
    return left + right


def smooth_row(above, row, below):
    near = beside(row)
    if above is not None:
        near = near + above
    if below is not None:
        near = near + below
    return row - 0.25 * near


def lanes_of(columns, sets):
    lane = lane_ids(sets)
    block = jnp.zeros((sets, LANES), F32)
    for slot, column in columns.items():
        block = jnp.where(lane == slot, column, block)
    return block


def pack(block):
    block = jnp.where(lane_ids(block.shape[0]) < SLOTS, block, 0.0)
    high = block.astype(BF16).astype(F32)
    rest = block - high
    mid = rest.astype(BF16).astype(F32)
    low = (rest - mid).astype(BF16).astype(F32)
    return (high + pltpu.roll(mid, SLOTS, 1) + pltpu.roll(low, 2 * SLOTS, 1)).astype(BF16)


def unpack(packed):
    block = packed.astype(F32)
    mid = pltpu.roll(block, LANES - SLOTS, 1)
    low = pltpu.roll(block, LANES - 2 * SLOTS, 1)
    return jnp.where(lane_ids(block.shape[0]) < SLOTS, (block + mid) + low, 0.0)


def row_of(values, index):
    return values[:, index * GRID : (index + 1) * GRID]


def seam(lower, upper):
    low0, low1, up0, up1 = row_of(lower, 0), row_of(lower, 1), row_of(upper, 0), row_of(upper, 1)
    cross = smooth_row(low0, low1, None) * up0 + smooth_row(None, up0, up1) * low1
    return jnp.sum(0.0625 * (up0 * up0 + low1 * low1) - 0.5 * cross, axis=1, keepdims=True)


def merge(mine_ref, got_ref, above, below, pixels, step, final, tile):
    upper_side = (tile // step) % 2 == 1
    inside = tile % step
    scalar_at = pl.ds(pixels, LANES)
    if mine_ref.dtype == F32:
        mine, got = mine_ref[:, scalar_at], got_ref[:, scalar_at]
    else:
        mine, got = unpack(mine_ref[:, scalar_at]), unpack(got_ref[:, scalar_at])
    edges, got_edges = mine_ref[:, pixels + LANES :].astype(F32), got_ref[:, pixels + LANES :].astype(F32)
    if final:
        first = last = None
        lower_last = jnp.where(upper_side, got_edges, edges)
        upper_first = jnp.where(upper_side, edges, got_edges)
    else:
        first = jnp.where(upper_side, got_edges[:, :EDGE], edges[:, :EDGE])
        last = jnp.where(upper_side, edges[:, EDGE:], got_edges[:, EDGE:])
        lower_last = jnp.where(upper_side, got_edges[:, EDGE:], edges[:, EDGE:])
        upper_first = jnp.where(upper_side, edges[:, :EDGE], got_edges[:, :EDGE])
    sets = mine.shape[0]
    scalars = mine + got + lanes_of({SMOOTH_SQ: seam(lower_last, upper_first)}, sets)
    above = jnp.where(upper_side & (inside == 0), lower_last, above)
    below = jnp.where(jnp.logical_not(upper_side) & (inside == step - 1), upper_first, below)
    value = mine_ref[:, :pixels].astype(F32) + got_ref[:, :pixels].astype(F32)
    return value, scalars, first, last, above, below


def edge_columns(step, n_par):
    return EDGE if 2 * step >= n_par else 2 * EDGE


def store_edges(message, at, first, last, step, n_par, tile):
    if 2 * step >= n_par:
        edges = jnp.where((tile // step) % 2 == 1, first, last)
    else:
        edges = jnp.concatenate([first, last], axis=1)
    message[:, at:] = edges.astype(message.dtype)


def own_columns(offset, width):
    return pl.ds(pl.multiple_of((lax.axis_index("pix") ^ offset) * width, LANES), width)


def store_block(block, sent, scalar):
    sets, width = sent.shape
    for r in range(width // LANES):
        block[r * sets : (r + 1) * sets, :] = sent[:, r * LANES : (r + 1) * LANES]
    if scalar is not None:
        diagonal = lax.broadcasted_iota(jnp.int32, (sets, LANES), 0) == lane_ids(sets)
        row = jnp.sum(jnp.where(diagonal, scalar, 0.0), axis=0, keepdims=True)
        high = row.astype(BF16).astype(F32)
        mid = (row - high).astype(BF16).astype(F32)
        low = row - high - mid
        line = lax.broadcasted_iota(jnp.int32, (TAIL, LANES), 0)
        tail = jnp.where(line == 0, high, jnp.where(line == 1, mid, jnp.where(line == 2, low, 0.0)))
        block[sets * width // LANES :, :] = tail.astype(BF16)


def load_block(block, sets, width):
    rows = width // LANES
    return jnp.concatenate([block[r * sets : (r + 1) * sets, :].astype(F32) for r in range(rows)], axis=1)


def load_scalar(block, sets, width):
    tail = block[sets * width // LANES :, :].astype(F32)
    row = (tail[0:1] + tail[1:2]) + tail[2:3]
    diagonal = lax.broadcasted_iota(jnp.int32, (sets, LANES), 0) == lane_ids(sets)
    return jnp.sum(jnp.where(diagonal, row, 0.0), axis=1, keepdims=True)


def shard_kernel(offset, n_shards, first_sweep, closing, n_par, *refs):
    refs = list(refs)
    shard, green = refs.pop(0), refs.pop(0)
    twice = None if first_sweep else refs.pop(0)
    image_in = refs.pop(0) if offset else None
    sets, width = shard.shape
    pixels = green.shape[1] if n_shards > 1 else green.shape[0]
    at = own_columns(offset, width) if n_shards > 1 else slice(None)
    value = shard[...]
    if n_shards > 1:
        image = jnp.dot(value, green[...], preferred_element_type=F32)
    else:
        image = lax.dot_general(value, green[...], (((1,), (1,)), ((), ())), preferred_element_type=F32)
    if image_in is not None:
        image += image_in[...]
    rows = width // GRID
    grad_sq = jnp.zeros((sets, LANES), F32)
    smooth_sq = jnp.zeros((sets, LANES), F32)
    cross = jnp.zeros((sets, LANES), F32)
    wide = value.astype(F32)
    beside_it = None if first_sweep else twice[:, at]
    for r in range(rows):
        row = row_of(wide, r)
        alone = smooth_row(row_of(wide, r - 1) if r else None, row, row_of(wide, r + 1) if r + 1 < rows else None)
        grad_sq += row * row
        smooth_sq += alone * alone
        if not first_sweep:
            cross += row * row_of(beside_it, r)
    columns = {GRAD_SQ: jnp.sum(grad_sq, axis=1, keepdims=True), SMOOTH_SQ: jnp.sum(smooth_sq, axis=1, keepdims=True)}
    if not first_sweep:
        columns[CROSS] = jnp.sum(cross, axis=1, keepdims=True)
    scalars = lanes_of(columns, sets)
    if not closing:
        refs[0][...] = image
        refs[1][...] = scalars
        return
    others, other_scalars = refs[: n_shards - 1], refs[n_shards - 1 : 2 * n_shards - 2]
    whole, message = refs[2 * n_shards - 2 :]
    cells = whole.shape[1]
    order = [k for k in range(n_shards) if k != offset]
    found = {offset: scalars}
    if n_shards > 1:
        whole[:, at] = value
    else:
        whole[...] = value
    for k, other, other_scalar in zip(order, others, other_scalars):
        whole[:, own_columns(k, width)] = other[...]
        found[k] = other_scalar[...]
    total = tree_sum([found[k] for k in range(n_shards)])
    seams = jnp.zeros((sets, 1), F32)
    for k in range(1, n_shards):
        edge = k * width
        seams += seam(whole[:, edge - EDGE : edge].astype(F32), whole[:, edge : edge + EDGE].astype(F32))
    message[:, :pixels] = image
    message[:, pixels : pixels + LANES] = total + lanes_of({SMOOTH_SQ: seams}, sets)
    first, last = whole[:, :EDGE].astype(F32), whole[:, cells - EDGE :].astype(F32)
    store_edges(message, pixels + LANES, first, last, 1, n_par, lax.axis_index("par"))


def middle_kernel(step, n_par, *refs):
    if step == 1:
        mine, got, message, above, below = refs
        old_above = old_below = jnp.zeros(above.shape, F32)
    else:
        mine, got, above_in, below_in, message, above, below = refs
        old_above, old_below = above_in[...], below_in[...]
    pixels = mine.shape[1] - LANES - 2 * EDGE
    tile = lax.axis_index("par")
    value, scalars, first, last, up, down = merge(mine, got, old_above, old_below, pixels, step, False, tile)
    message[:, :pixels] = value.astype(BF16)
    message[:, pixels : pixels + LANES] = pack(scalars)
    store_edges(message, pixels + LANES, first, last, 2 * step, n_par, tile)
    above[...] = up
    below[...] = down


def image_kernel(step, n_pix, first_sweep, has_block, keep_rounded, *refs):
    refs = list(refs)
    mine, got, above_in, below_in = (refs.pop(0) for _ in range(4))
    old_scalars, old_image = (None, None) if first_sweep else (refs.pop(0), refs.pop(0))
    green, lost = (refs.pop(0), refs.pop(0)) if has_block else (None, None)
    scalars, image, above, below = (refs.pop(0) for _ in range(4))
    rounded = refs.pop(0) if keep_rounded else None
    sets, pixels = image.shape
    value, sums, _, _, up, down = merge(
        mine, got, above_in[...], below_in[...], pixels, step, True, lax.axis_index("par")
    )
    above[...] = up
    below[...] = down
    grad_sq = sums[:, GRAD_SQ : GRAD_SQ + 1]
    smooth_sq = sums[:, SMOOTH_SQ : SMOOTH_SQ + 1]
    beta = jnp.zeros((sets, 1), F32)
    if not first_sweep:
        beta = grad_sq / old_scalars[:, GRAD_SQ : GRAD_SQ + 1]
        old_smooth = old_scalars[:, SMOOTH_SQ : SMOOTH_SQ + 1]
        smooth_sq = smooth_sq + beta * (2.0 * sums[:, CROSS : CROSS + 1] + beta * old_smooth)
        value = value + beta * old_image[...]
    image[...] = value
    if keep_rounded:
        rounded[...] = value.astype(BF16)
    image_sq = jnp.zeros((sets, LANES), F32)
    for at in range(0, pixels, LANES):
        part = value[:, at : at + LANES]
        image_sq += part * part
    image_sq = jnp.sum(image_sq, axis=1, keepdims=True)
    guess = (n_pix * image_sq + smooth_sq) / grad_sq
    scalars[...] = lanes_of(
        {GRAD_SQ: grad_sq, SMOOTH_SQ: smooth_sq, IMAGE_SQ: image_sq, BETA: beta, GUESS: guess}, sets
    )
    if has_block:
        send_block(send_order(n_pix)[0], value.astype(BF16), green, lost.shape[1], lost, guess, image_sq, *refs)


def send_block(offset, image, green, width, lost, guess, image_sq, block, missed=None):
    part = jnp.dot(image, green[:, own_columns(offset, width)], preferred_element_type=F32)
    aimed = part if lost is None else part - guess * lost[...]
    sent = aimed.astype(BF16)
    store_block(block, sent, image_sq)
    if missed is not None:
        missed[...] = part - sent.astype(F32)


def block_kernel(offset, rounded, scalars, green, lost, *refs):
    guess, image_sq = scalars[:, GUESS : GUESS + 1], scalars[:, IMAGE_SQ : IMAGE_SQ + 1]
    send_block(offset, rounded[...], green, lost.shape[1], lost, guess, image_sq, *refs)


def own_kernel(first_sweep, n_par, direct, has_product, *refs):
    refs = list(refs)
    scalars, above, below, whole = (refs.pop(0) for _ in range(4))
    old_direction = None if first_sweep else refs.pop(0)
    rounded, green = (refs.pop(0), refs.pop(0)) if has_product else (None, None)
    direction = refs.pop(0)
    cells = whole.shape[1]
    rows = cells // GRID
    if first_sweep:
        direction[:, :EDGE] = above[...]
        direction[:, EDGE : EDGE + cells] = whole[...].astype(F32)
        direction[:, EDGE + cells :] = below[...]
    else:
        beta = scalars[:, BETA : BETA + 1]
        direction[:, :EDGE] = above[...] + beta * old_direction[:, :EDGE]
        direction[:, EDGE : EDGE + cells] = whole[...].astype(F32) + beta * old_direction[:, EDGE : EDGE + cells]
        direction[:, EDGE + cells :] = below[...] + beta * old_direction[:, EDGE + cells :]
    if not has_product:
        return
    twice, own, once = refs
    tile = lax.axis_index("par")

    def from_ref(ref, r):
        return ref[:, r * GRID : (r + 1) * GRID]

    for r in range(rows + 2):
        row = smooth_row(from_ref(direction, r), from_ref(direction, r + 1), from_ref(direction, r + 2))
        if r == 0:
            row = jnp.where(tile == 0, 0.0, row)
        if r == rows + 1:
            row = jnp.where(tile == n_par - 1, 0.0, row)
        once[:, r * GRID : (r + 1) * GRID] = row
    for r in range(rows):
        row = smooth_row(from_ref(once, r), from_ref(once, r + 1), from_ref(once, r + 2))
        twice[:, r * GRID : (r + 1) * GRID] = row
    if direct:
        at = own_columns(0, own.shape[1])
        own[...] = jnp.dot(rounded[...], green[:, at], preferred_element_type=F32) + twice[:, at]
    else:
        own[...] = jnp.dot(rounded[...], green[...], preferred_element_type=F32)


def start_kernel(observed_at, green_at, green, own, *refs):
    refs, (observed, observed_sem, sems) = refs[:-3], refs[-3:]
    n_pix = len(refs) // 2 + 1
    width = own.shape[1]
    order = send_order(n_pix) + [0]
    first = pltpu.make_async_copy(observed_at, observed, observed_sem)
    first.start()
    copies = []
    for i, offset in enumerate(order):
        at = own_columns(offset, width)
        copies.append(pltpu.make_async_copy(green_at.at[:, at], green.at[:, at], sems.at[i]))
        copies[-1].start()
    first.wait()
    image = observed[...]
    for i, offset in enumerate(order):
        copies[i].wait()
        if offset:
            send_block(offset, image, green, width, None, None, None, refs[i], refs[n_pix - 1 + i])
        else:
            own[...] = jnp.dot(image, green[:, own_columns(0, width)], preferred_element_type=F32)


def turn_kernel(offset, green, turned):
    turned[...] = green[:, own_columns(offset, turned.shape[0])].T


def receive_start_kernel(count, own, *refs):
    got, (grad, rounded) = refs[: count - 1], refs[-2:]
    sets, width = own.shape
    value = tree_sum(by_offset(count, own[...], [load_block(ref, sets, width) for ref in got]))
    grad[...] = value
    rounded[...] = value.astype(BF16)


def step_length(scalars, others):
    own = scalars[:, IMAGE_SQ : IMAGE_SQ + 1]
    image_sq = tree_sum(by_offset(len(others) + 1, own, others))
    return scalars[:, GRAD_SQ : GRAD_SQ + 1] / (image_sq + scalars[:, SMOOTH_SQ : SMOOTH_SQ + 1])


def receive_kernel(keep_grad, own, scalars, old_grad, *refs):
    refs, grad = (refs[:-1], refs[-1]) if keep_grad else (refs, None)
    got, (rounded, length) = refs[:-2], refs[-2:]
    sets, width = own.shape
    step_len = step_length(scalars, [load_scalar(ref, sets, width) for ref in got])
    change = tree_sum(by_offset(len(got) + 1, own[...], [load_block(ref, sets, width) for ref in got]))
    value = old_grad[...] - step_len * change
    if keep_grad:
        grad[...] = value
    rounded[...] = value.astype(BF16)
    length[...] = jnp.broadcast_to(step_len, length.shape)


def update_kernel(count, length, direction, image, solution, residual, *refs):
    step_len = length[:, :1]
    lost, missed = refs[:count], refs[count : 2 * count]
    new_solution, new_residual = refs[2 * count : 2 * count + 2]
    for old, change, new in zip(lost, missed, refs[2 * count + 2 :]):
        new[...] = old[...] - step_len * change[...]
    cells = solution.shape[1]
    new_solution[...] = solution[...] + step_len * direction[:, EDGE : EDGE + cells]
    new_residual[...] = residual[...] - step_len * image[...]


def finish_kernel(scalars, *refs):
    got, (direction, image, solution, residual, new_solution, new_residual) = refs[:-6], refs[-6:]
    step_len = step_length(scalars, [ref[:, IMAGE_SQ : IMAGE_SQ + 1] for ref in got])
    cells = solution.shape[1]
    new_solution[...] = solution[...] + step_len * direction[:, EDGE : EDGE + cells]
    new_residual[...] = residual[...] - step_len * image[...]


def call(kernel, operands, outs, scratch=(), flops=0, limit=24 << 20, space=pltpu.VMEM):
    vmem = pl.BlockSpec(memory_space=pltpu.VMEM)
    shapes = [jax.ShapeDtypeStruct(*out) if isinstance(out, tuple) else out for out in outs]
    moved = sum(math.prod(x.shape) * jnp.dtype(x.dtype).itemsize for x in [*operands, *shapes])
    return pl.pallas_call(
        kernel,
        in_specs=[pl.BlockSpec(memory_space=space)] * len(operands),
        out_specs=[vmem] * len(outs),
        out_shape=shapes,
        scratch_shapes=list(scratch),
        name=getattr(kernel, "func", kernel).__name__,
        compiler_params=pltpu.CompilerParams(vmem_limit_bytes=limit),
        cost_estimate=pl.CostEstimate(flops=flops or moved, bytes_accessed=moved, transcendentals=0),
    )(*operands)


def exchange(blocks, axis, count):
    return {k: lax.ppermute(block, axis, xor_pairs(count, k)) for k, block in blocks.items()}


def by_offset(count, own, got):
    found = {0: own, **dict(zip(send_order(count), got))}
    return [found[k] for k in range(count)]


def on_device(green, observed):
    sets = observed.shape[0]
    pixels, cells = green.shape
    n_pix, n_par = lax.axis_size("pix"), lax.axis_size("par")
    here = lax.axis_index("pix")
    width = cells // n_pix
    direct = n_pix <= 8 and width % LANES == 0
    flops = 2 * sets * pixels * cells
    part_flops = flops // n_pix
    count = n_pix - 1 if direct else 0
    shard, rounded_shard = ((sets, width), F32), ((sets, width), BF16)
    plain = ((sets * width // LANES, LANES), BF16)
    block = ((sets * width // LANES + TAIL, LANES), BF16)
    scalar = ((sets, LANES), F32)
    line, wide, edge = ((sets, pixels), F32), ((sets, cells), F32), ((sets, EDGE), F32)
    ring = ((sets, cells + 2 * EDGE), F32)

    order = send_order(n_pix) if direct else []
    turn = gather_order(n_pix) if direct else []
    lost, got = {}, {}
    if direct:
        green, own, *rest = call(
            start_kernel,
            [observed, green],
            [pltpu.VMEM(*out) for out in [(green.shape, BF16), shard] + [plain] * count + [shard] * count],
            [pltpu.VMEM(observed.shape, BF16), pltpu.SemaphoreType.DMA, pltpu.SemaphoreType.DMA((n_pix,))],
            flops,
            limit=48 << 20,
            space=pltpu.HBM,
        )
        lost = dict(zip(order, rest[count:]))
        turned_shape = ((width, pixels), BF16)
        turned = {k: call(functools.partial(turn_kernel, k), [green], [turned_shape])[0] for k in [0] + turn}
        got = exchange(dict(zip(order, rest)), "pix", n_pix)
        ready = turned.values()
    else:
        turned, ready = {0: green}, []
        partial = jnp.dot(observed, green, preferred_element_type=F32)
        own = lax.psum_scatter(partial, "pix", scatter_dimension=1, tiled=True)
    grad, rounded_grad = call(
        functools.partial(receive_start_kernel, len(got) + 1),
        [own, *got.values(), *ready],
        [shard, rounded_shard],
    )
    solution = jnp.zeros((sets, cells), F32)
    residual = observed.astype(F32)
    scalars = image = direction = twice = None
    for sweep in range(ITERS):
        first, final = sweep == 0, sweep + 1 == ITERS
        if direct:
            shards = {0: rounded_grad, **exchange(dict.fromkeys(turn, rounded_grad), "pix", n_pix)}
        else:
            shards = {0: lax.all_gather(rounded_grad, "pix", axis=1, tiled=True)}
        beside_them = [] if first else [twice]

        def message_of(step):
            return ((sets, pixels + LANES + edge_columns(step, n_par)), F32 if step == 1 else BF16)

        partial, parts = [], {}
        closing = ([0] + turn)[-1]
        for k in ([0] + turn)[:-1]:
            kernel = functools.partial(shard_kernel, k, len(shards), first, False, n_par)
            out, parts[k] = call(kernel, [shards[k], turned[k], *beside_them, *partial], [line, scalar], flops=part_flops)
            partial = [out]
        others = sorted(parts)
        whole, message = call(
            functools.partial(shard_kernel, closing, len(shards), first, True, n_par),
            [shards[closing], turned[closing], *beside_them, *partial]
            + [shards[o] for o in others]
            + [parts[o] for o in others],
            [((sets, cells), BF16), message_of(1)],
            flops=part_flops,
        )
        step, above, below = 1, None, None
        while True:
            got = lax.ppermute(message, "par", xor_pairs(n_par, step))
            if 2 * step >= n_par:
                break
            message, above, below = call(
                functools.partial(middle_kernel, step, n_par),
                [message, got, *([] if step == 1 else [above, below])],
                [message_of(2 * step), edge, edge],
            )
            step *= 2
        if above is None:
            above = below = jnp.zeros(edge[0], F32)
        has_block = direct and not final
        again = sweep + 2 < ITERS
        blocks, missed = {}, {}
        sent = [block, shard] if again else [block]
        scalars, image, above, below, *rest = call(
            functools.partial(image_kernel, step, n_pix, first, has_block, not final),
            [message, got, above, below]
            + ([] if first else [scalars, image])
            + ([green, lost[order[0]]] if has_block else []),
            [scalar, line, edge, edge]
            + ([] if final else [((sets, pixels), BF16)])
            + (sent if has_block else []),
            flops=part_flops if has_block else 0,
        )
        olds = [] if first else [direction]
        if final:
            (direction,) = call(
                functools.partial(own_kernel, first, n_par, direct, False),
                [scalars, above, below, whole, *olds],
                [ring],
            )
            if direct:
                got = exchange(dict.fromkeys(order, scalars), "pix", n_pix)
            else:
                got = {}
                scalars = scalars.at[:, IMAGE_SQ].set(lax.psum(scalars[:, IMAGE_SQ], "pix"))
            return tuple(call(finish_kernel, [scalars, *got.values(), direction, image, solution, residual], [wide, line]))
        rounded, *rest = rest
        if direct:
            blocks[order[0]], missed[order[0]] = rest[0], rest[1:]
            for k in order[1:]:
                blocks[k], *missed[k] = call(
                    functools.partial(block_kernel, k),
                    [rounded, scalars, green, lost[k]],
                    sent,
                    flops=part_flops,
                )
        direction, twice, own = call(
            functools.partial(own_kernel, first, n_par, direct, True),
            [scalars, above, below, whole, *olds, rounded, green],
            [ring, wide, shard if direct else wide],
            [pltpu.VMEM((sets, cells + EDGE), F32)],
            part_flops if direct else flops,
        )
        if direct:
            got = exchange(blocks, "pix", n_pix)
        else:
            got = {}
            own = lax.psum_scatter(own, "pix", scatter_dimension=1, tiled=True)
            own = own + lax.dynamic_slice_in_dim(twice, here * width, width, axis=1)
            scalars = scalars.at[:, IMAGE_SQ].set(lax.psum(scalars[:, IMAGE_SQ], "pix"))
        rounded_grad, length, *rest = call(
            functools.partial(receive_kernel, again),
            [own, scalars, grad, *got.values()],
            [rounded_shard, scalar] + ([shard] if again else []),
        )
        (grad,) = rest or (None,)
        solution, residual, *rest = call(
            functools.partial(update_kernel, count if again else 0),
            [length, direction, image, solution, residual]
            + ([*lost.values(), *(one for (one,) in missed.values())] if again else []),
            [wide, line] + ([shard] * count if again else []),
        )
        lost = dict(zip(order, rest))


def solution(mesh):
    return jax.shard_map(
        on_device,
        mesh=mesh,
        in_specs=(P("pix", "par"), P("parts", "pix")),
        out_specs=(P("parts", "par"), P("parts", "pix")),
        check_vma=False,
    )
```

```python
import functools
import math

import jax
import jax.numpy as jnp
from jax import lax
from jax.experimental import pallas as pl
from jax.experimental.pallas import tpu as pltpu
from jax.sharding import PartitionSpec as P

GRID = 128
ITERS = 5
LANES = 128
EDGE = 2 * GRID
SLOTS = 8
TAIL = 8
BF16 = jnp.bfloat16
F32 = jnp.float32

GRAD_SQ, SMOOTH_SQ, CROSS = 0, 1, 2
IMAGE_SQ, BETA, GUESS = 2, 3, 4


def xor_pairs(count, offset):
    return [(i, i ^ offset) for i in range(count)]


def send_order(count):
    half = count // 2
    return [half] + [k for k in range(count - 1, 0, -1) if k != half]


def gather_order(count):
    half = count // 2
    return [half] + [k for k in range(1, count) if k != half]


def tree_sum(parts):
    while len(parts) > 1:
        parts = [parts[i] + parts[i + 1] for i in range(0, len(parts), 2)]
    return parts[0]


def lane_ids(sets):
    return lax.broadcasted_iota(jnp.int32, (sets, LANES), 1)


def beside(row):
    lane = lane_ids(row.shape[0])
    left = jnp.where(lane == 0, 0.0, pltpu.roll(row, 1, 1))
    right = jnp.where(lane == LANES - 1, 0.0, pltpu.roll(row, LANES - 1, 1))
    return left + right


def smooth_row(above, row, below):
    near = beside(row)
    if above is not None:
        near = near + above
    if below is not None:
        near = near + below
    return row - 0.25 * near


def lanes_of(columns, sets):
    lane = lane_ids(sets)
    block = jnp.zeros((sets, LANES), F32)
    for slot, column in columns.items():
        block = jnp.where(lane == slot, column, block)
    return block


def pack(block):
    block = jnp.where(lane_ids(block.shape[0]) < SLOTS, block, 0.0)
    high = block.astype(BF16).astype(F32)
    rest = block - high
    mid = rest.astype(BF16).astype(F32)
    low = (rest - mid).astype(BF16).astype(F32)
    return (high + pltpu.roll(mid, SLOTS, 1) + pltpu.roll(low, 2 * SLOTS, 1)).astype(BF16)


def unpack(packed):
    block = packed.astype(F32)
    mid = pltpu.roll(block, LANES - SLOTS, 1)
    low = pltpu.roll(block, LANES - 2 * SLOTS, 1)
    return jnp.where(lane_ids(block.shape[0]) < SLOTS, (block + mid) + low, 0.0)


def row_of(values, index):
    return values[:, index * GRID : (index + 1) * GRID]


def seam(lower, upper):
    low0, low1, up0, up1 = row_of(lower, 0), row_of(lower, 1), row_of(upper, 0), row_of(upper, 1)
    cross = smooth_row(low0, low1, None) * up0 + smooth_row(None, up0, up1) * low1
    return jnp.sum(0.0625 * (up0 * up0 + low1 * low1) - 0.5 * cross, axis=1, keepdims=True)


def merge_sums(mine_ref, got_ref, pixels):
    scalar_at = pl.ds(pixels, LANES)
    if mine_ref.dtype == F32:
        scalars = mine_ref[:, scalar_at] + got_ref[:, scalar_at]
    else:
        scalars = unpack(mine_ref[:, scalar_at]) + unpack(got_ref[:, scalar_at])
    return mine_ref[:, :pixels].astype(F32) + got_ref[:, :pixels].astype(F32), scalars


def merge_edges(mine_ref, got_ref, above, below, pixels, step, final, tile):
    upper_side = (tile // step) % 2 == 1
    inside = tile % step
    edges, got_edges = mine_ref[:, pixels + LANES :].astype(F32), got_ref[:, pixels + LANES :].astype(F32)
    if final:
        first = last = None
        lower_last = jnp.where(upper_side, got_edges, edges)
        upper_first = jnp.where(upper_side, edges, got_edges)
    else:
        first = jnp.where(upper_side, got_edges[:, :EDGE], edges[:, :EDGE])
        last = jnp.where(upper_side, edges[:, EDGE:], got_edges[:, EDGE:])
        lower_last = jnp.where(upper_side, got_edges[:, EDGE:], edges[:, EDGE:])
        upper_first = jnp.where(upper_side, edges[:, :EDGE], got_edges[:, :EDGE])
    above = jnp.where(upper_side & (inside == 0), lower_last, above)
    below = jnp.where(jnp.logical_not(upper_side) & (inside == step - 1), upper_first, below)
    return seam(lower_last, upper_first), first, last, above, below


def edge_columns(step, n_par):
    return EDGE if 2 * step >= n_par else 2 * EDGE


def store_edges(message, at, first, last, step, n_par, tile):
    if 2 * step >= n_par:
        edges = jnp.where((tile // step) % 2 == 1, first, last)
    else:
        edges = jnp.concatenate([first, last], axis=1)
    message[:, at:] = edges.astype(message.dtype)


def own_columns(offset, width):
    return pl.ds(pl.multiple_of((lax.axis_index("pix") ^ offset) * width, LANES), width)


def store_block(block, sent, scalar):
    sets, width = sent.shape
    for r in range(width // LANES):
        block[r * sets : (r + 1) * sets, :] = sent[:, r * LANES : (r + 1) * LANES]
    if scalar is not None:
        diagonal = lax.broadcasted_iota(jnp.int32, (sets, LANES), 0) == lane_ids(sets)
        row = jnp.sum(jnp.where(diagonal, scalar, 0.0), axis=0, keepdims=True)
        high = row.astype(BF16).astype(F32)
        mid = (row - high).astype(BF16).astype(F32)
        low = row - high - mid
        line = lax.broadcasted_iota(jnp.int32, (TAIL, LANES), 0)
        tail = jnp.where(line == 0, high, jnp.where(line == 1, mid, jnp.where(line == 2, low, 0.0)))
        block[sets * width // LANES :, :] = tail.astype(BF16)


def load_block(block, sets, width):
    rows = width // LANES
    return jnp.concatenate([block[r * sets : (r + 1) * sets, :].astype(F32) for r in range(rows)], axis=1)


def load_scalar(block, sets, width):
    tail = block[sets * width // LANES :, :].astype(F32)
    row = (tail[0:1] + tail[1:2]) + tail[2:3]
    diagonal = lax.broadcasted_iota(jnp.int32, (sets, LANES), 0) == lane_ids(sets)
    return jnp.sum(jnp.where(diagonal, row, 0.0), axis=1, keepdims=True)


def shard_kernel(offset, n_shards, first_sweep, closing, n_par, *refs):
    refs = list(refs)
    shard, green = refs.pop(0), refs.pop(0)
    twice = None if first_sweep else refs.pop(0)
    image_in = refs.pop(0) if offset else None
    sets, width = shard.shape
    pixels = green.shape[1] if n_shards > 1 else green.shape[0]
    at = own_columns(offset, width) if n_shards > 1 else slice(None)
    value = shard[...]
    if n_shards > 1:
        image = jnp.dot(value, green[...], preferred_element_type=F32)
    else:
        image = lax.dot_general(value, green[...], (((1,), (1,)), ((), ())), preferred_element_type=F32)
    if image_in is not None:
        image += image_in[...]
    rows = width // GRID
    grad_sq = jnp.zeros((sets, LANES), F32)
    smooth_sq = jnp.zeros((sets, LANES), F32)
    cross = jnp.zeros((sets, LANES), F32)
    wide = value.astype(F32)
    beside_it = None if first_sweep else twice[:, at]
    for r in range(rows):
        row = row_of(wide, r)
        alone = smooth_row(row_of(wide, r - 1) if r else None, row, row_of(wide, r + 1) if r + 1 < rows else None)
        grad_sq += row * row
        smooth_sq += alone * alone
        if not first_sweep:
            cross += row * row_of(beside_it, r)
    columns = {GRAD_SQ: jnp.sum(grad_sq, axis=1, keepdims=True), SMOOTH_SQ: jnp.sum(smooth_sq, axis=1, keepdims=True)}
    if not first_sweep:
        columns[CROSS] = jnp.sum(cross, axis=1, keepdims=True)
    scalars = lanes_of(columns, sets)
    if not closing:
        refs[0][...] = image
        refs[1][...] = scalars
        return
    others, other_scalars = refs[: n_shards - 1], refs[n_shards - 1 : 2 * n_shards - 2]
    whole, message = refs[2 * n_shards - 2 :]
    cells = whole.shape[1]
    order = [k for k in range(n_shards) if k != offset]
    found = {offset: scalars}
    if n_shards > 1:
        whole[:, at] = value
    else:
        whole[...] = value
    for k, other, other_scalar in zip(order, others, other_scalars):
        whole[:, own_columns(k, width)] = other[...]
        found[k] = other_scalar[...]
    total = tree_sum([found[k] for k in range(n_shards)])
    seams = jnp.zeros((sets, 1), F32)
    for k in range(1, n_shards):
        edge = k * width
        seams += seam(whole[:, edge - EDGE : edge].astype(F32), whole[:, edge : edge + EDGE].astype(F32))
    message[:, :pixels] = image
    message[:, pixels : pixels + LANES] = total + lanes_of({SMOOTH_SQ: seams}, sets)
    first, last = whole[:, :EDGE].astype(F32), whole[:, cells - EDGE :].astype(F32)
    store_edges(message, pixels + LANES, first, last, 1, n_par, lax.axis_index("par"))


def middle_kernel(step, n_par, *refs):
    if step == 1:
        mine, got, message, above, below = refs
        old_above = old_below = jnp.zeros(above.shape, F32)
    else:
        mine, got, above_in, below_in, message, above, below = refs
        old_above, old_below = above_in[...], below_in[...]
    pixels = mine.shape[1] - LANES - 2 * EDGE
    tile = lax.axis_index("par")
    value, scalars = merge_sums(mine, got, pixels)
    added, first, last, up, down = merge_edges(mine, got, old_above, old_below, pixels, step, False, tile)
    scalars += lanes_of({SMOOTH_SQ: added}, value.shape[0])
    message[:, :pixels] = value.astype(BF16)
    message[:, pixels : pixels + LANES] = pack(scalars)
    store_edges(message, pixels + LANES, first, last, 2 * step, n_par, tile)
    above[...] = up
    below[...] = down


def image_kernel(n_pix, first_sweep, early, keep_rounded, *refs):
    refs = list(refs)
    mine, got = refs.pop(0), refs.pop(0)
    old_scalars, old_image = (None, None) if first_sweep else (refs.pop(0), refs.pop(0))
    green = refs.pop(0) if early else None
    lost = [refs.pop(0) for _ in early]
    scalars, image = refs.pop(0), refs.pop(0)
    rounded = refs.pop(0) if keep_rounded else None
    sets, pixels = image.shape
    value, sums = merge_sums(mine, got, pixels)
    grad_sq = sums[:, GRAD_SQ : GRAD_SQ + 1]
    smooth_sq = sums[:, SMOOTH_SQ : SMOOTH_SQ + 1]
    beta = jnp.zeros((sets, 1), F32)
    if not first_sweep:
        beta = grad_sq / old_scalars[:, GRAD_SQ : GRAD_SQ + 1]
        old_smooth = old_scalars[:, SMOOTH_SQ : SMOOTH_SQ + 1]
        smooth_sq = smooth_sq + beta * (2.0 * sums[:, CROSS : CROSS + 1] + beta * old_smooth)
        value = value + beta * old_image[...]
    image[...] = value
    if keep_rounded:
        rounded[...] = value.astype(BF16)
    image_sq = jnp.zeros((sets, LANES), F32)
    for at in range(0, pixels, LANES):
        part = value[:, at : at + LANES]
        image_sq += part * part
    image_sq = jnp.sum(image_sq, axis=1, keepdims=True)
    guess = (n_pix * image_sq + jnp.maximum(smooth_sq, 0.0)) / grad_sq
    scalars[...] = lanes_of(
        {GRAD_SQ: grad_sq, SMOOTH_SQ: smooth_sq, IMAGE_SQ: image_sq, BETA: beta, GUESS: guess}, sets
    )
    each = len(refs) // len(early) if early else 0
    for i, offset in enumerate(early):
        outs = refs[i * each : (i + 1) * each]
        send_block(offset, value.astype(BF16), green, lost[i].shape[1], lost[i], guess, image_sq, *outs)


def send_block(offset, image, green, width, lost, guess, image_sq, block, missed=None):
    part = jnp.dot(image, green[:, own_columns(offset, width)], preferred_element_type=F32)
    aimed = part if lost is None else part - guess * lost[...]
    sent = aimed.astype(BF16)
    store_block(block, sent, image_sq)
    if missed is not None:
        missed[...] = part - sent.astype(F32)


def block_kernel(offset, rounded, scalars, green, lost, *refs):
    guess, image_sq = scalars[:, GUESS : GUESS + 1], scalars[:, IMAGE_SQ : IMAGE_SQ + 1]
    send_block(offset, rounded[...], green, lost.shape[1], lost, guess, image_sq, *refs)


def own_kernel(step, first_sweep, n_par, direct, has_product, *refs):
    refs = list(refs)
    sums, mine, got, above_in, below_in, whole = (refs.pop(0) for _ in range(6))
    old_direction = None if first_sweep else refs.pop(0)
    rounded, green = (refs.pop(0), refs.pop(0)) if has_product else (None, None)
    scalars, direction = refs.pop(0), refs.pop(0)
    sets, cells = whole.shape
    rows = cells // GRID
    tile = lax.axis_index("par")
    pixels = mine.shape[1] - LANES - EDGE
    added, _, _, above, below = merge_edges(mine, got, above_in[...], below_in[...], pixels, step, True, tile)
    scalars[...] = sums[...] + lanes_of({SMOOTH_SQ: added}, sets)
    if first_sweep:
        direction[:, :EDGE] = above
        direction[:, EDGE : EDGE + cells] = whole[...].astype(F32)
        direction[:, EDGE + cells :] = below
    else:
        beta = sums[:, BETA : BETA + 1]
        direction[:, :EDGE] = above + beta * old_direction[:, :EDGE]
        direction[:, EDGE : EDGE + cells] = whole[...].astype(F32) + beta * old_direction[:, EDGE : EDGE + cells]
        direction[:, EDGE + cells :] = below + beta * old_direction[:, EDGE + cells :]
    if not has_product:
        return
    twice, own, once = refs

    def from_ref(ref, r):
        return ref[:, r * GRID : (r + 1) * GRID]

    for r in range(rows + 2):
        row = smooth_row(from_ref(direction, r), from_ref(direction, r + 1), from_ref(direction, r + 2))
        if r == 0:
            row = jnp.where(tile == 0, 0.0, row)
        if r == rows + 1:
            row = jnp.where(tile == n_par - 1, 0.0, row)
        once[:, r * GRID : (r + 1) * GRID] = row
    for r in range(rows):
        row = smooth_row(from_ref(once, r), from_ref(once, r + 1), from_ref(once, r + 2))
        twice[:, r * GRID : (r + 1) * GRID] = row
    if direct:
        at = own_columns(0, own.shape[1])
        own[...] = jnp.dot(rounded[...], green[:, at], preferred_element_type=F32) + twice[:, at]
    else:
        own[...] = jnp.dot(rounded[...], green[...], preferred_element_type=F32)


def start_kernel(observed_at, green_at, green, own, *refs):
    refs, (observed, observed_sem, sems) = refs[:-3], refs[-3:]
    n_pix = len(refs) // 2 + 1
    width = own.shape[1]
    order = send_order(n_pix) + [0]
    first = pltpu.make_async_copy(observed_at, observed, observed_sem)
    first.start()
    copies = []
    for i, offset in enumerate(order):
        at = own_columns(offset, width)
        copies.append(pltpu.make_async_copy(green_at.at[:, at], green.at[:, at], sems.at[i]))
        copies[-1].start()
    first.wait()
    image = observed[...]
    for i, offset in enumerate(order):
        copies[i].wait()
        if offset:
            send_block(offset, image, green, width, None, None, None, refs[i], refs[n_pix - 1 + i])
        else:
            own[...] = jnp.dot(image, green[:, own_columns(0, width)], preferred_element_type=F32)


def turn_kernel(offset, green, turned):
    turned[...] = green[:, own_columns(offset, turned.shape[0])].T


def receive_start_kernel(count, own, *refs):
    got, (grad, rounded) = refs[: count - 1], refs[-2:]
    sets, width = own.shape
    value = tree_sum(by_offset(count, own[...], [load_block(ref, sets, width) for ref in got]))
    grad[...] = value
    rounded[...] = value.astype(BF16)


def step_length(scalars, others):
    own = scalars[:, IMAGE_SQ : IMAGE_SQ + 1]
    image_sq = tree_sum(by_offset(len(others) + 1, own, others))
    return scalars[:, GRAD_SQ : GRAD_SQ + 1] / (image_sq + scalars[:, SMOOTH_SQ : SMOOTH_SQ + 1])


def receive_kernel(keep_grad, own, scalars, old_grad, *refs):
    refs, grad = (refs[:-1], refs[-1]) if keep_grad else (refs, None)
    got, (rounded, length) = refs[:-2], refs[-2:]
    sets, width = own.shape
    step_len = step_length(scalars, [load_scalar(ref, sets, width) for ref in got])
    change = tree_sum(by_offset(len(got) + 1, own[...], [load_block(ref, sets, width) for ref in got]))
    value = old_grad[...] - step_len * change
    if keep_grad:
        grad[...] = value
    rounded[...] = value.astype(BF16)
    length[...] = jnp.broadcast_to(step_len, length.shape)


def update_kernel(count, length, direction, image, solution, residual, *refs):
    step_len = length[:, :1]
    lost, missed = refs[:count], refs[count : 2 * count]
    new_solution, new_residual = refs[2 * count : 2 * count + 2]
    for old, change, new in zip(lost, missed, refs[2 * count + 2 :]):
        new[...] = old[...] - step_len * change[...]
    cells = solution.shape[1]
    new_solution[...] = solution[...] + step_len * direction[:, EDGE : EDGE + cells]
    new_residual[...] = residual[...] - step_len * image[...]


def finish_kernel(scalars, *refs):
    got, (direction, image, solution, residual, new_solution, new_residual) = refs[:-6], refs[-6:]
    step_len = step_length(scalars, [ref[:, IMAGE_SQ : IMAGE_SQ + 1] for ref in got])
    cells = solution.shape[1]
    new_solution[...] = solution[...] + step_len * direction[:, EDGE : EDGE + cells]
    new_residual[...] = residual[...] - step_len * image[...]


def call(kernel, operands, outs, scratch=(), flops=0, limit=24 << 20, space=pltpu.VMEM):
    vmem = pl.BlockSpec(memory_space=pltpu.VMEM)
    shapes = [jax.ShapeDtypeStruct(*out) if isinstance(out, tuple) else out for out in outs]
    moved = sum(math.prod(x.shape) * jnp.dtype(x.dtype).itemsize for x in [*operands, *shapes])
    return pl.pallas_call(
        kernel,
        in_specs=[pl.BlockSpec(memory_space=space)] * len(operands),
        out_specs=[vmem] * len(outs),
        out_shape=shapes,
        scratch_shapes=list(scratch),
        name=getattr(kernel, "func", kernel).__name__,
        compiler_params=pltpu.CompilerParams(vmem_limit_bytes=limit),
        cost_estimate=pl.CostEstimate(flops=flops or moved, bytes_accessed=moved, transcendentals=0),
    )(*operands)


def exchange(blocks, axis, count):
    return {k: lax.ppermute(block, axis, xor_pairs(count, k)) for k, block in blocks.items()}


def by_offset(count, own, got):
    found = {0: own, **dict(zip(send_order(count), got))}
    return [found[k] for k in range(count)]


def on_device(green, observed):
    sets = observed.shape[0]
    pixels, cells = green.shape
    n_pix, n_par = lax.axis_size("pix"), lax.axis_size("par")
    here = lax.axis_index("pix")
    width = cells // n_pix
    direct = n_pix <= 8 and width % LANES == 0
    flops = 2 * sets * pixels * cells
    part_flops = flops // n_pix
    count = n_pix - 1 if direct else 0
    shard, rounded_shard = ((sets, width), F32), ((sets, width), BF16)
    plain = ((sets * width // LANES, LANES), BF16)
    block = ((sets * width // LANES + TAIL, LANES), BF16)
    scalar = ((sets, LANES), F32)
    line, wide, edge = ((sets, pixels), F32), ((sets, cells), F32), ((sets, EDGE), F32)
    ring = ((sets, cells + 2 * EDGE), F32)

    order = send_order(n_pix) if direct else []
    turn = gather_order(n_pix) if direct else []
    lost, got = {}, {}
    if direct:
        green, own, *rest = call(
            start_kernel,
            [observed, green],
            [pltpu.VMEM(*out) for out in [(green.shape, BF16), shard] + [plain] * count + [shard] * count],
            [pltpu.VMEM(observed.shape, BF16), pltpu.SemaphoreType.DMA, pltpu.SemaphoreType.DMA((n_pix,))],
            flops,
            limit=48 << 20,
            space=pltpu.HBM,
        )
        lost = dict(zip(order, rest[count:]))
        turned_shape = ((width, pixels), BF16)
        turned = {k: call(functools.partial(turn_kernel, k), [green], [turned_shape])[0] for k in [0] + turn}
        got = exchange(dict(zip(order, rest)), "pix", n_pix)
        ready = turned.values()
    else:
        turned, ready = {0: green}, []
        partial = jnp.dot(observed, green, preferred_element_type=F32)
        own = lax.psum_scatter(partial, "pix", scatter_dimension=1, tiled=True)
    grad, rounded_grad = call(
        functools.partial(receive_start_kernel, len(got) + 1),
        [own, *got.values(), *ready],
        [shard, rounded_shard],
    )
    solution = jnp.zeros((sets, cells), F32)
    residual = observed.astype(F32)
    scalars = image = direction = twice = None
    for sweep in range(ITERS):
        first, final = sweep == 0, sweep + 1 == ITERS
        if direct:
            shards = {0: rounded_grad, **exchange(dict.fromkeys(turn, rounded_grad), "pix", n_pix)}
        else:
            shards = {0: lax.all_gather(rounded_grad, "pix", axis=1, tiled=True)}
        beside_them = [] if first else [twice]

        def message_of(step):
            return ((sets, pixels + LANES + edge_columns(step, n_par)), F32 if step == 1 else BF16)

        partial, parts = [], {}
        closing = ([0] + turn)[-1]
        for k in ([0] + turn)[:-1]:
            kernel = functools.partial(shard_kernel, k, len(shards), first, False, n_par)
            out, parts[k] = call(kernel, [shards[k], turned[k], *beside_them, *partial], [line, scalar], flops=part_flops)
            partial = [out]
        others = sorted(parts)
        whole, message = call(
            functools.partial(shard_kernel, closing, len(shards), first, True, n_par),
            [shards[closing], turned[closing], *beside_them, *partial]
            + [shards[o] for o in others]
            + [parts[o] for o in others],
            [((sets, cells), BF16), message_of(1)],
            flops=part_flops,
        )
        step, above, below = 1, None, None
        while True:
            got = lax.ppermute(message, "par", xor_pairs(n_par, step))
            if 2 * step >= n_par:
                break
            message, above, below = call(
                functools.partial(middle_kernel, step, n_par),
                [message, got, *([] if step == 1 else [above, below])],
                [message_of(2 * step), edge, edge],
            )
            step *= 2
        if above is None:
            above = below = jnp.zeros(edge[0], F32)
        again = sweep + 2 < ITERS
        early = [] if final else order[:1]
        blocks, missed = {}, {}
        sent = [block, shard] if again else [block]
        sums, image, *rest = call(
            functools.partial(image_kernel, n_pix, first, early, not final),
            [message, got]
            + ([] if first else [scalars, image])
            + ([green] if early else [])
            + [lost[k] for k in early],
            [scalar, line] + ([] if final else [((sets, pixels), BF16)]) + sent * len(early),
            flops=part_flops * len(early),
        )
        ends = [sums, message, got, above, below, whole, *([] if first else [direction])]
        if final:
            scalars, direction = call(
                functools.partial(own_kernel, step, first, n_par, direct, False), ends, [scalar, ring]
            )
            if direct:
                got = exchange(dict.fromkeys(order, sums), "pix", n_pix)
            else:
                got = {}
                scalars = scalars.at[:, IMAGE_SQ].set(lax.psum(scalars[:, IMAGE_SQ], "pix"))
            return tuple(call(finish_kernel, [scalars, *got.values(), direction, image, solution, residual], [wide, line]))
        rounded, *rest = rest
        if direct:
            for i, k in enumerate(early):
                blocks[k], *missed[k] = rest[i * len(sent) : (i + 1) * len(sent)]
            for k in order[len(early) :]:
                blocks[k], *missed[k] = call(
                    functools.partial(block_kernel, k),
                    [rounded, sums, green, lost[k]],
                    sent,
                    flops=part_flops,
                )
        scalars, direction, twice, own = call(
            functools.partial(own_kernel, step, first, n_par, direct, True),
            [*ends, rounded, green],
            [scalar, ring, wide, shard if direct else wide],
            [pltpu.VMEM((sets, cells + EDGE), F32)],
            part_flops if direct else flops,
        )
        if direct:
            got = exchange(blocks, "pix", n_pix)
        else:
            got = {}
            own = lax.psum_scatter(own, "pix", scatter_dimension=1, tiled=True)
            own = own + lax.dynamic_slice_in_dim(twice, here * width, width, axis=1)
            scalars = scalars.at[:, IMAGE_SQ].set(lax.psum(scalars[:, IMAGE_SQ], "pix"))
        rounded_grad, length, *rest = call(
            functools.partial(receive_kernel, again),
            [own, scalars, grad, *got.values()],
            [rounded_shard, scalar] + ([shard] if again else []),
        )
        (grad,) = rest or (None,)
        solution, residual, *rest = call(
            functools.partial(update_kernel, count if again else 0),
            [length, direction, image, solution, residual]
            + ([*lost.values(), *(one for (one,) in missed.values())] if again else []),
            [wide, line] + ([shard] * count if again else []),
        )
        lost = dict(zip(order, rest))


def solution(mesh):
    return jax.shard_map(
        on_device,
        mesh=mesh,
        in_specs=(P("pix", "par"), P("parts", "pix")),
        out_specs=(P("parts", "par"), P("parts", "pix")),
        check_vma=False,
    )
```

```python
import functools
import math

import jax
import jax.numpy as jnp
from jax import lax
from jax.experimental import pallas as pl
from jax.experimental.pallas import tpu as pltpu
from jax.sharding import PartitionSpec as P

GRID = 128
ITERS = 5
LANES = 128
EDGE = 2 * GRID
SLOTS = 8
TAIL = 8
BF16 = jnp.bfloat16
F32 = jnp.float32

GRAD_SQ, SMOOTH_SQ, CROSS = 0, 1, 2
IMAGE_SQ, BETA, GUESS = 2, 3, 4


def xor_pairs(count, offset):
    return [(i, i ^ offset) for i in range(count)]


def send_order(count):
    half = count // 2
    return [half] + [k for k in range(count - 1, 0, -1) if k != half]


def gather_order(count):
    half = count // 2
    return [half] + [k for k in range(1, count) if k != half]


def tree_sum(parts):
    while len(parts) > 1:
        parts = [parts[i] + parts[i + 1] for i in range(0, len(parts), 2)]
    return parts[0]


def lane_ids(sets):
    return lax.broadcasted_iota(jnp.int32, (sets, LANES), 1)


def beside(row):
    lane = lane_ids(row.shape[0])
    left = jnp.where(lane == 0, 0.0, pltpu.roll(row, 1, 1))
    right = jnp.where(lane == LANES - 1, 0.0, pltpu.roll(row, LANES - 1, 1))
    return left + right


def smooth_row(above, row, below):
    near = beside(row)
    if above is not None:
        near = near + above
    if below is not None:
        near = near + below
    return row - 0.25 * near


def lanes_of(columns, sets):
    lane = lane_ids(sets)
    block = jnp.zeros((sets, LANES), F32)
    for slot, column in columns.items():
        block = jnp.where(lane == slot, column, block)
    return block


def pack(block):
    block = jnp.where(lane_ids(block.shape[0]) < SLOTS, block, 0.0)
    high = block.astype(BF16).astype(F32)
    rest = block - high
    mid = rest.astype(BF16).astype(F32)
    low = (rest - mid).astype(BF16).astype(F32)
    return (high + pltpu.roll(mid, SLOTS, 1) + pltpu.roll(low, 2 * SLOTS, 1)).astype(BF16)


def unpack(packed):
    block = packed.astype(F32)
    mid = pltpu.roll(block, LANES - SLOTS, 1)
    low = pltpu.roll(block, LANES - 2 * SLOTS, 1)
    return jnp.where(lane_ids(block.shape[0]) < SLOTS, (block + mid) + low, 0.0)


def row_of(values, index):
    return values[:, index * GRID : (index + 1) * GRID]


def seam(lower, upper):
    low0, low1, up0, up1 = row_of(lower, 0), row_of(lower, 1), row_of(upper, 0), row_of(upper, 1)
    cross = smooth_row(low0, low1, None) * up0 + smooth_row(None, up0, up1) * low1
    return jnp.sum(0.0625 * (up0 * up0 + low1 * low1) - 0.5 * cross, axis=1, keepdims=True)


def merge_sums(mine_ref, got_ref, pixels):
    scalar_at = pl.ds(pixels, LANES)
    scalars = unpack(mine_ref[:, scalar_at]) + unpack(got_ref[:, scalar_at])
    return mine_ref[:, :pixels].astype(F32) + got_ref[:, :pixels].astype(F32), scalars


def merge_edges(mine_ref, got_ref, above, below, pixels, step, final, tile):
    upper_side = (tile // step) % 2 == 1
    inside = tile % step
    edges, got_edges = mine_ref[:, pixels + LANES :].astype(F32), got_ref[:, pixels + LANES :].astype(F32)
    if final:
        first = last = None
        lower_last = jnp.where(upper_side, got_edges, edges)
        upper_first = jnp.where(upper_side, edges, got_edges)
    else:
        first = jnp.where(upper_side, got_edges[:, :EDGE], edges[:, :EDGE])
        last = jnp.where(upper_side, edges[:, EDGE:], got_edges[:, EDGE:])
        lower_last = jnp.where(upper_side, got_edges[:, EDGE:], edges[:, EDGE:])
        upper_first = jnp.where(upper_side, edges[:, :EDGE], got_edges[:, :EDGE])
    above = jnp.where(upper_side & (inside == 0), lower_last, above)
    below = jnp.where(jnp.logical_not(upper_side) & (inside == step - 1), upper_first, below)
    return seam(lower_last, upper_first), first, last, above, below


def edge_columns(step, n_par):
    return EDGE if 2 * step >= n_par else 2 * EDGE


def store_edges(message, at, first, last, step, n_par, tile):
    if 2 * step >= n_par:
        edges = jnp.where((tile // step) % 2 == 1, first, last)
    else:
        edges = jnp.concatenate([first, last], axis=1)
    message[:, at:] = edges.astype(message.dtype)


def own_columns(offset, width):
    return pl.ds(pl.multiple_of((lax.axis_index("pix") ^ offset) * width, LANES), width)


def store_block(block, sent, scalar):
    sets, width = sent.shape
    for r in range(width // LANES):
        block[r * sets : (r + 1) * sets, :] = sent[:, r * LANES : (r + 1) * LANES]
    if scalar is not None:
        diagonal = lax.broadcasted_iota(jnp.int32, (sets, LANES), 0) == lane_ids(sets)
        row = jnp.sum(jnp.where(diagonal, scalar, 0.0), axis=0, keepdims=True)
        high = row.astype(BF16).astype(F32)
        mid = (row - high).astype(BF16).astype(F32)
        low = row - high - mid
        line = lax.broadcasted_iota(jnp.int32, (TAIL, LANES), 0)
        tail = jnp.where(line == 0, high, jnp.where(line == 1, mid, jnp.where(line == 2, low, 0.0)))
        block[sets * width // LANES :, :] = tail.astype(BF16)


def load_block(block, sets, width):
    rows = width // LANES
    return jnp.concatenate([block[r * sets : (r + 1) * sets, :].astype(F32) for r in range(rows)], axis=1)


def load_scalar(block, sets, width):
    tail = block[sets * width // LANES :, :].astype(F32)
    row = (tail[0:1] + tail[1:2]) + tail[2:3]
    diagonal = lax.broadcasted_iota(jnp.int32, (sets, LANES), 0) == lane_ids(sets)
    return jnp.sum(jnp.where(diagonal, row, 0.0), axis=1, keepdims=True)


def shard_kernel(offset, n_shards, first_sweep, closing, n_par, *refs):
    refs = list(refs)
    shard, green = refs.pop(0), refs.pop(0)
    twice = None if first_sweep else refs.pop(0)
    image_in = refs.pop(0) if offset else None
    sets, width = shard.shape
    pixels = green.shape[1] if n_shards > 1 else green.shape[0]
    at = own_columns(offset, width) if n_shards > 1 else slice(None)
    value = shard[...]
    if n_shards > 1:
        image = jnp.dot(value, green[...], preferred_element_type=F32)
    else:
        image = lax.dot_general(value, green[...], (((1,), (1,)), ((), ())), preferred_element_type=F32)
    if image_in is not None:
        image += image_in[...]
    rows = width // GRID
    grad_sq = jnp.zeros((sets, LANES), F32)
    smooth_sq = jnp.zeros((sets, LANES), F32)
    cross = jnp.zeros((sets, LANES), F32)
    wide = value.astype(F32)
    beside_it = None if first_sweep else twice[:, at]
    for r in range(rows):
        row = row_of(wide, r)
        alone = smooth_row(row_of(wide, r - 1) if r else None, row, row_of(wide, r + 1) if r + 1 < rows else None)
        grad_sq += row * row
        smooth_sq += alone * alone
        if not first_sweep:
            cross += row * row_of(beside_it, r)
    columns = {GRAD_SQ: jnp.sum(grad_sq, axis=1, keepdims=True), SMOOTH_SQ: jnp.sum(smooth_sq, axis=1, keepdims=True)}
    if not first_sweep:
        columns[CROSS] = jnp.sum(cross, axis=1, keepdims=True)
    scalars = lanes_of(columns, sets)
    if not closing:
        refs[0][...] = image
        refs[1][...] = scalars
        return
    others, other_scalars = refs[: n_shards - 1], refs[n_shards - 1 : 2 * n_shards - 2]
    whole, message = refs[2 * n_shards - 2 :]
    cells = whole.shape[1]
    order = [k for k in range(n_shards) if k != offset]
    found = {offset: scalars}
    if n_shards > 1:
        whole[:, at] = value
    else:
        whole[...] = value
    for k, other, other_scalar in zip(order, others, other_scalars):
        whole[:, own_columns(k, width)] = other[...]
        found[k] = other_scalar[...]
    total = tree_sum([found[k] for k in range(n_shards)])
    seams = jnp.zeros((sets, 1), F32)
    for k in range(1, n_shards):
        edge = k * width
        seams += seam(whole[:, edge - EDGE : edge].astype(F32), whole[:, edge : edge + EDGE].astype(F32))
    message[:, :pixels] = image.astype(BF16)
    message[:, pixels : pixels + LANES] = pack(total + lanes_of({SMOOTH_SQ: seams}, sets))
    first, last = whole[:, :EDGE].astype(F32), whole[:, cells - EDGE :].astype(F32)
    store_edges(message, pixels + LANES, first, last, 1, n_par, lax.axis_index("par"))


def middle_kernel(step, n_par, *refs):
    if step == 1:
        mine, got, message, above, below = refs
        old_above = old_below = jnp.zeros(above.shape, F32)
    else:
        mine, got, above_in, below_in, message, above, below = refs
        old_above, old_below = above_in[...], below_in[...]
    pixels = mine.shape[1] - LANES - 2 * EDGE
    tile = lax.axis_index("par")
    value, scalars = merge_sums(mine, got, pixels)
    added, first, last, up, down = merge_edges(mine, got, old_above, old_below, pixels, step, False, tile)
    scalars += lanes_of({SMOOTH_SQ: added}, value.shape[0])
    message[:, :pixels] = value.astype(BF16)
    message[:, pixels : pixels + LANES] = pack(scalars)
    store_edges(message, pixels + LANES, first, last, 2 * step, n_par, tile)
    above[...] = up
    below[...] = down


def image_kernel(n_pix, first_sweep, early, keep_rounded, *refs):
    refs = list(refs)
    mine, got = refs.pop(0), refs.pop(0)
    old_scalars, old_image = (None, None) if first_sweep else (refs.pop(0), refs.pop(0))
    green = refs.pop(0) if early else None
    lost = [refs.pop(0) for _ in early]
    scalars, image = refs.pop(0), refs.pop(0)
    rounded = refs.pop(0) if keep_rounded else None
    sets, pixels = image.shape
    value, sums = merge_sums(mine, got, pixels)
    grad_sq = sums[:, GRAD_SQ : GRAD_SQ + 1]
    smooth_sq = sums[:, SMOOTH_SQ : SMOOTH_SQ + 1]
    beta = jnp.zeros((sets, 1), F32)
    if not first_sweep:
        beta = grad_sq / old_scalars[:, GRAD_SQ : GRAD_SQ + 1]
        old_smooth = old_scalars[:, SMOOTH_SQ : SMOOTH_SQ + 1]
        smooth_sq = smooth_sq + beta * (2.0 * sums[:, CROSS : CROSS + 1] + beta * old_smooth)
        value = value + beta * old_image[...]
    image[...] = value
    if keep_rounded:
        rounded[...] = value.astype(BF16)
    image_sq = jnp.zeros((sets, LANES), F32)
    for at in range(0, pixels, LANES):
        part = value[:, at : at + LANES]
        image_sq += part * part
    image_sq = jnp.sum(image_sq, axis=1, keepdims=True)
    guess = (n_pix * image_sq + jnp.maximum(smooth_sq, 0.0)) / grad_sq
    scalars[...] = lanes_of(
        {GRAD_SQ: grad_sq, SMOOTH_SQ: smooth_sq, IMAGE_SQ: image_sq, BETA: beta, GUESS: guess}, sets
    )
    each = len(refs) // len(early) if early else 0
    for i, offset in enumerate(early):
        outs = refs[i * each : (i + 1) * each]
        send_block(offset, value.astype(BF16), green, lost[i].shape[1], lost[i], guess, image_sq, *outs)


def send_block(offset, image, green, width, lost, guess, image_sq, block, missed=None):
    part = jnp.dot(image, green[:, own_columns(offset, width)], preferred_element_type=F32)
    aimed = part if lost is None else part - guess * lost[...]
    sent = aimed.astype(BF16)
    store_block(block, sent, image_sq)
    if missed is not None:
        missed[...] = part - sent.astype(F32)


def block_kernel(offset, rounded, scalars, green, lost, *refs):
    guess, image_sq = scalars[:, GUESS : GUESS + 1], scalars[:, IMAGE_SQ : IMAGE_SQ + 1]
    send_block(offset, rounded[...], green, lost.shape[1], lost, guess, image_sq, *refs)


def own_kernel(step, first_sweep, n_par, direct, has_product, *refs):
    refs = list(refs)
    sums, mine, got, above_in, below_in, whole = (refs.pop(0) for _ in range(6))
    old_direction = None if first_sweep else refs.pop(0)
    rounded, green = (refs.pop(0), refs.pop(0)) if has_product else (None, None)
    scalars, direction = refs.pop(0), refs.pop(0)
    sets, cells = whole.shape
    rows = cells // GRID
    tile = lax.axis_index("par")
    pixels = mine.shape[1] - LANES - EDGE
    added, _, _, above, below = merge_edges(mine, got, above_in[...], below_in[...], pixels, step, True, tile)
    scalars[...] = sums[...] + lanes_of({SMOOTH_SQ: added}, sets)
    if first_sweep:
        direction[:, :EDGE] = above
        direction[:, EDGE : EDGE + cells] = whole[...].astype(F32)
        direction[:, EDGE + cells :] = below
    else:
        beta = sums[:, BETA : BETA + 1]
        direction[:, :EDGE] = above + beta * old_direction[:, :EDGE]
        direction[:, EDGE : EDGE + cells] = whole[...].astype(F32) + beta * old_direction[:, EDGE : EDGE + cells]
        direction[:, EDGE + cells :] = below + beta * old_direction[:, EDGE + cells :]
    if not has_product:
        return
    twice, own, once = refs

    def from_ref(ref, r):
        return ref[:, r * GRID : (r + 1) * GRID]

    for r in range(rows + 2):
        row = smooth_row(from_ref(direction, r), from_ref(direction, r + 1), from_ref(direction, r + 2))
        if r == 0:
            row = jnp.where(tile == 0, 0.0, row)
        if r == rows + 1:
            row = jnp.where(tile == n_par - 1, 0.0, row)
        once[:, r * GRID : (r + 1) * GRID] = row
    for r in range(rows):
        row = smooth_row(from_ref(once, r), from_ref(once, r + 1), from_ref(once, r + 2))
        twice[:, r * GRID : (r + 1) * GRID] = row
    if direct:
        at = own_columns(0, own.shape[1])
        own[...] = jnp.dot(rounded[...], green[:, at], preferred_element_type=F32) + twice[:, at]
    else:
        own[...] = jnp.dot(rounded[...], green[...], preferred_element_type=F32)


def start_kernel(observed_at, green_at, green, own, *refs):
    refs, (observed, observed_sem, sems) = refs[:-3], refs[-3:]
    n_pix = len(refs) // 2 + 1
    width = own.shape[1]
    order = send_order(n_pix) + [0]
    first = pltpu.make_async_copy(observed_at, observed, observed_sem)
    first.start()
    copies = []
    for i, offset in enumerate(order):
        at = own_columns(offset, width)
        copies.append(pltpu.make_async_copy(green_at.at[:, at], green.at[:, at], sems.at[i]))
        copies[-1].start()
    first.wait()
    image = observed[...]
    for i, offset in enumerate(order):
        copies[i].wait()
        if offset:
            send_block(offset, image, green, width, None, None, None, refs[i], refs[n_pix - 1 + i])
        else:
            own[...] = jnp.dot(image, green[:, own_columns(0, width)], preferred_element_type=F32)


def turn_kernel(offset, green, turned):
    turned[...] = green[:, own_columns(offset, turned.shape[0])].T


def receive_start_kernel(count, own, *refs):
    got, (grad, rounded) = refs[: count - 1], refs[-2:]
    sets, width = own.shape
    value = tree_sum(by_offset(count, own[...], [load_block(ref, sets, width) for ref in got]))
    grad[...] = value
    rounded[...] = value.astype(BF16)


def step_length(scalars, others):
    own = scalars[:, IMAGE_SQ : IMAGE_SQ + 1]
    image_sq = tree_sum(by_offset(len(others) + 1, own, others))
    return scalars[:, GRAD_SQ : GRAD_SQ + 1] / (image_sq + scalars[:, SMOOTH_SQ : SMOOTH_SQ + 1])


def receive_kernel(keep_grad, own, scalars, old_grad, *refs):
    refs, grad = (refs[:-1], refs[-1]) if keep_grad else (refs, None)
    got, (rounded, length) = refs[:-2], refs[-2:]
    sets, width = own.shape
    step_len = step_length(scalars, [load_scalar(ref, sets, width) for ref in got])
    change = tree_sum(by_offset(len(got) + 1, own[...], [load_block(ref, sets, width) for ref in got]))
    value = old_grad[...] - step_len * change
    if keep_grad:
        grad[...] = value
    rounded[...] = value.astype(BF16)
    length[...] = jnp.broadcast_to(step_len, length.shape)


def update_kernel(count, length, direction, image, solution, residual, *refs):
    step_len = length[:, :1]
    lost, missed = refs[:count], refs[count : 2 * count]
    new_solution, new_residual = refs[2 * count : 2 * count + 2]
    for old, change, new in zip(lost, missed, refs[2 * count + 2 :]):
        new[...] = old[...] - step_len * change[...]
    cells = solution.shape[1]
    new_solution[...] = solution[...] + step_len * direction[:, EDGE : EDGE + cells]
    new_residual[...] = residual[...] - step_len * image[...]


def finish_kernel(scalars, *refs):
    got, (direction, image, solution, residual, new_solution, new_residual) = refs[:-6], refs[-6:]
    step_len = step_length(scalars, [ref[:, IMAGE_SQ : IMAGE_SQ + 1] for ref in got])
    cells = solution.shape[1]
    new_solution[...] = solution[...] + step_len * direction[:, EDGE : EDGE + cells]
    new_residual[...] = residual[...] - step_len * image[...]


def call(kernel, operands, outs, scratch=(), flops=0, limit=24 << 20, space=pltpu.VMEM):
    vmem = pl.BlockSpec(memory_space=pltpu.VMEM)
    shapes = [jax.ShapeDtypeStruct(*out) if isinstance(out, tuple) else out for out in outs]
    moved = sum(math.prod(x.shape) * jnp.dtype(x.dtype).itemsize for x in [*operands, *shapes])
    return pl.pallas_call(
        kernel,
        in_specs=[pl.BlockSpec(memory_space=space)] * len(operands),
        out_specs=[vmem] * len(outs),
        out_shape=shapes,
        scratch_shapes=list(scratch),
        name=getattr(kernel, "func", kernel).__name__,
        compiler_params=pltpu.CompilerParams(vmem_limit_bytes=limit),
        cost_estimate=pl.CostEstimate(flops=flops or moved, bytes_accessed=moved, transcendentals=0),
    )(*operands)


def exchange(blocks, axis, count):
    return {k: lax.ppermute(block, axis, xor_pairs(count, k)) for k, block in blocks.items()}


def by_offset(count, own, got):
    found = {0: own, **dict(zip(send_order(count), got))}
    return [found[k] for k in range(count)]


def on_device(green, observed):
    sets = observed.shape[0]
    pixels, cells = green.shape
    n_pix, n_par = lax.axis_size("pix"), lax.axis_size("par")
    here = lax.axis_index("pix")
    width = cells // n_pix
    direct = n_pix <= 8 and width % LANES == 0
    flops = 2 * sets * pixels * cells
    part_flops = flops // n_pix
    count = n_pix - 1 if direct else 0
    shard, rounded_shard = ((sets, width), F32), ((sets, width), BF16)
    plain = ((sets * width // LANES, LANES), BF16)
    block = ((sets * width // LANES + TAIL, LANES), BF16)
    scalar = ((sets, LANES), F32)
    line, wide, edge = ((sets, pixels), F32), ((sets, cells), F32), ((sets, EDGE), F32)
    ring = ((sets, cells + 2 * EDGE), F32)

    order = send_order(n_pix) if direct else []
    turn = gather_order(n_pix) if direct else []
    lost, got = {}, {}
    if direct:
        green, own, *rest = call(
            start_kernel,
            [observed, green],
            [pltpu.VMEM(*out) for out in [(green.shape, BF16), shard] + [plain] * count + [shard] * count],
            [pltpu.VMEM(observed.shape, BF16), pltpu.SemaphoreType.DMA, pltpu.SemaphoreType.DMA((n_pix,))],
            flops,
            limit=48 << 20,
            space=pltpu.HBM,
        )
        lost = dict(zip(order, rest[count:]))
        turned_shape = ((width, pixels), BF16)
        turned = {k: call(functools.partial(turn_kernel, k), [green], [turned_shape])[0] for k in [0] + turn}
        got = exchange(dict(zip(order, rest)), "pix", n_pix)
        ready = turned.values()
    else:
        turned, ready = {0: green}, []
        partial = jnp.dot(observed, green, preferred_element_type=F32)
        own = lax.psum_scatter(partial, "pix", scatter_dimension=1, tiled=True)
    grad, rounded_grad = call(
        functools.partial(receive_start_kernel, len(got) + 1),
        [own, *got.values(), *ready],
        [shard, rounded_shard],
    )
    solution = jnp.zeros((sets, cells), F32)
    residual = observed.astype(F32)
    scalars = image = direction = twice = None
    for sweep in range(ITERS):
        first, final = sweep == 0, sweep + 1 == ITERS
        if direct:
            shards = {0: rounded_grad, **exchange(dict.fromkeys(turn, rounded_grad), "pix", n_pix)}
        else:
            shards = {0: lax.all_gather(rounded_grad, "pix", axis=1, tiled=True)}
        beside_them = [] if first else [twice]

        def message_of(step):
            return ((sets, pixels + LANES + edge_columns(step, n_par)), BF16)

        partial, parts = [], {}
        closing = ([0] + turn)[-1]
        for k in ([0] + turn)[:-1]:
            kernel = functools.partial(shard_kernel, k, len(shards), first, False, n_par)
            out, parts[k] = call(kernel, [shards[k], turned[k], *beside_them, *partial], [line, scalar], flops=part_flops)
            partial = [out]
        others = sorted(parts)
        whole, message = call(
            functools.partial(shard_kernel, closing, len(shards), first, True, n_par),
            [shards[closing], turned[closing], *beside_them, *partial]
            + [shards[o] for o in others]
            + [parts[o] for o in others],
            [((sets, cells), BF16), message_of(1)],
            flops=part_flops,
        )
        step, above, below = 1, None, None
        while True:
            got = lax.ppermute(message, "par", xor_pairs(n_par, step))
            if 2 * step >= n_par:
                break
            message, above, below = call(
                functools.partial(middle_kernel, step, n_par),
                [message, got, *([] if step == 1 else [above, below])],
                [message_of(2 * step), edge, edge],
            )
            step *= 2
        if above is None:
            above = below = jnp.zeros(edge[0], F32)
        again = sweep + 2 < ITERS
        early = [] if final else order[:1]
        blocks, missed = {}, {}
        sent = [block, shard] if again else [block]
        sums, image, *rest = call(
            functools.partial(image_kernel, n_pix, first, early, not final),
            [message, got]
            + ([] if first else [scalars, image])
            + ([green] if early else [])
            + [lost[k] for k in early],
            [scalar, line] + ([] if final else [((sets, pixels), BF16)]) + sent * len(early),
            flops=part_flops * len(early),
        )
        ends = [sums, message, got, above, below, whole, *([] if first else [direction])]
        if final:
            scalars, direction = call(
                functools.partial(own_kernel, step, first, n_par, direct, False), ends, [scalar, ring]
            )
            if direct:
                got = exchange(dict.fromkeys(order, sums), "pix", n_pix)
            else:
                got = {}
                scalars = scalars.at[:, IMAGE_SQ].set(lax.psum(scalars[:, IMAGE_SQ], "pix"))
            return tuple(call(finish_kernel, [scalars, *got.values(), direction, image, solution, residual], [wide, line]))
        rounded, *rest = rest
        if direct:
            for i, k in enumerate(early):
                blocks[k], *missed[k] = rest[i * len(sent) : (i + 1) * len(sent)]
            for k in order[len(early) :]:
                blocks[k], *missed[k] = call(
                    functools.partial(block_kernel, k),
                    [rounded, sums, green, lost[k]],
                    sent,
                    flops=part_flops,
                )
        scalars, direction, twice, own = call(
            functools.partial(own_kernel, step, first, n_par, direct, True),
            [*ends, rounded, green],
            [scalar, ring, wide, shard if direct else wide],
            [pltpu.VMEM((sets, cells + EDGE), F32)],
            part_flops if direct else flops,
        )
        if direct:
            got = exchange(blocks, "pix", n_pix)
        else:
            got = {}
            own = lax.psum_scatter(own, "pix", scatter_dimension=1, tiled=True)
            own = own + lax.dynamic_slice_in_dim(twice, here * width, width, axis=1)
            scalars = scalars.at[:, IMAGE_SQ].set(lax.psum(scalars[:, IMAGE_SQ], "pix"))
        rounded_grad, length, *rest = call(
            functools.partial(receive_kernel, again),
            [own, scalars, grad, *got.values()],
            [rounded_shard, scalar] + ([shard] if again else []),
        )
        (grad,) = rest or (None,)
        solution, residual, *rest = call(
            functools.partial(update_kernel, count if again else 0),
            [length, direction, image, solution, residual]
            + ([*lost.values(), *(one for (one,) in missed.values())] if again else []),
            [wide, line] + ([shard] * count if again else []),
        )
        lost = dict(zip(order, rest))


def solution(mesh):
    return jax.shard_map(
        on_device,
        mesh=mesh,
        in_specs=(P("pix", "par"), P("parts", "pix")),
        out_specs=(P("parts", "par"), P("parts", "pix")),
        check_vma=False,
    )
```
